256 devices in a mesh: dp: 2 (over x_lo), fsdp: 16 (over x_hi, y, core), tensor: 8 (over z).
Axes of the slice: x: 4 (x_hi: 2, x_lo: 2; x = x_hi * 2 + x_lo), y: 4, z: 8, core: 2. Of those that a mesh axis runs over, the one named last changes fastest.
Arguments:
- hidden: bfloat16 [16384, 2048], P(('dp', 'fsdp'), 'tensor'), may hold values from -8 to 8
- norm_gain: bfloat16 [2048], P('tensor'), may hold values from 0.099609375 to 1.8984375
- head_weight: bfloat16 [2048, 32128], P('fsdp', 'tensor'), may hold values from -1 to 1
- token_ids: int32 [32, 512], P(('dp', 'fsdp')), may hold values from 0 to 32127
- lengths: int32 [32], P(('dp', 'fsdp')), may hold values from 128 to 512
- old_logp: float32 [32, 512], P(('dp', 'fsdp')), may hold values from -12.5 to -9.5
- advantages: float32 [32, 512], P(('dp', 'fsdp')), may hold values from -4 to 4
- rollout_logp: float32 [32, 512], P(('dp', 'fsdp'), 'tensor'), may hold values from -16 to -1
- rollout_row: int32 [32], P(('dp', 'fsdp')), may hold values from 0 to 31, each once
Outputs:
- new_logp: float32 [32, 512], P(('dp', 'fsdp'))
- token_loss: float32 [32, 512], P(('dp', 'fsdp'))
- summary: float32 [3], replicated
The draws below stay inside these ranges and needn't reach their ends.
Inputs may be any that keep to these rules, and one draw needn't show every extreme that they name: `rollout_row`: every row 0 to 31 is named once.
All inputs are finite; a program needn't handle non-finite values.
Results may differ from the reference program's by a relative error of at most 0.0005.
The reference program's roundings to bfloat16 on the way (of `normed`) count: a program that leaves them out, or rounds other values in their place, can miss the bound.
Values may be sent and summed in bfloat16 or wider, within the bound.
A program may use at most 128 MiB of HBM per device.

```python
import math
import jax
import jax.numpy as jnp
import numpy as np
from jax import lax

D = 2048
VOCAB = 32128
LEN = 512
RESP = 32
TOKENS = 16384


def draw_hidden(key, part):
    samples = jax.random.normal(jax.random.fold_in(key, 21), (TOKENS, D), jnp.float32)
    return jnp.clip(samples, -8.0, 8.0).astype(jnp.bfloat16)


def draw_head_weight(key, part):
    weights = jax.random.normal(jax.random.fold_in(key, 31), (D, VOCAB), jnp.float32) / math.sqrt(D)
    return jnp.clip(weights, -1.0, 1.0).astype(jnp.bfloat16)


def draw_lengths(key, part):
    row_index = jnp.arange(RESP, dtype=jnp.int32)
    shortest = LEN // 4
    rising = shortest + row_index * (LEN - shortest) // max(RESP - 1, 1)
    jitter = jax.random.randint(jax.random.fold_in(key, 41), (RESP,), 0, LEN // 8 + 1)
    values = jnp.clip(rising - jitter, shortest, LEN)
    values = jnp.where(row_index == RESP - 1, LEN, values)
    values = jnp.where(row_index == 0, shortest, values)
    return values.astype(jnp.int32)


def draw_rollout_logp(key, part):
    center = -math.log(VOCAB)
    row_offset = jax.random.uniform(jax.random.fold_in(key, 51), (RESP, 1), jnp.float32, -2.0, 2.0)
    token_jitter = jax.random.uniform(jax.random.fold_in(key, 52), (RESP, LEN), jnp.float32, -1.0, 1.0)
    return jnp.clip(center + row_offset + token_jitter, -16.0, -1.0)


def with_ends(array, rng, smallest, largest):
    longest = array.shape.index(max(array.shape))
    spots = []
    for shift in (0, 1):
        where = [jax.random.randint(jax.random.fold_in(rng, axis), (), 0, length) for axis, length in enumerate(array.shape)]
        where[longest] = (where[longest] + shift) % array.shape[longest]
        spots.append(tuple(where))
    return array.at[spots[0]].set(smallest).at[spots[1]].set(largest)


def block_levels(key, dims, cuts, low, high):
    loudness, own = 1.0, jax.random.fold_in(key, 6)
    for dim, parts in cuts:
        draws = jnp.exp(jax.random.uniform(jax.random.fold_in(own, dim), (parts,), jnp.float32, low / len(cuts), high / len(cuts)))
        loudness = loudness * jnp.repeat(draws, dims[dim] // parts).reshape([-1 if axis == dim else 1 for axis in range(len(dims))])
    return loudness


def cumulative_ranks(amount, slope):
    portions = [(1 << 20) // math.isqrt(rank ** slope) + 1 for rank in range(1, amount + 1)]
    deviation = 1 + sum(portions) // (1 << 30)
    return np.cumsum(np.array([max(1, weight // deviation) for weight in portions]))


def ranked_ids(stream_key, extent, amount, skew):
    listing = cumulative_ranks(amount, skew)
    lot = jax.random.randint(jax.random.fold_in(stream_key, 1), extent, 0, int(listing[amount - 1]))
    standing = jnp.searchsorted(jnp.asarray(listing, jnp.int32), lot, side="right")
    return jax.random.permutation(jax.random.fold_in(stream_key, 2), amount)[standing].astype(jnp.int32)


def noise(own_key, extent, deviation, most, cuts=(), kind=jnp.bfloat16):
    drawn = jax.random.normal(own_key, extent, jnp.float32) * deviation
    if len(cuts) > 0:
        drawn = block_levels(own_key, extent, cuts, -0.22, 0.18) * drawn
    return jnp.clip(drawn, min=-most, max=most).astype(kind)


def setup_inputs(seed: int = 0) -> dict:
    splits = jax.random.split(jax.random.key(seed), 10)
    hidden = draw_hidden(jax.random.fold_in(splits[9], 71), 0)
    norm_gain = jnp.clip(1.0 + 0.18 * jax.random.normal(splits[1], (D,), jnp.float32), 0.099609375, 1.8984375).astype(jnp.bfloat16)
    head_weight = draw_head_weight(jax.random.fold_in(splits[9], 71), 0)
    token_ids = with_ends(ranked_ids(splits[3], (RESP, LEN), VOCAB, 2), jax.random.fold_in(splits[3], 3), 0, VOCAB - 1).astype(jnp.int32)
    lengths = draw_lengths(jax.random.fold_in(splits[9], 71), 0)
    old_logp = jnp.clip(-12.5 + 3.0 * jax.random.uniform(splits[5], (RESP, LEN), jnp.float32) ** block_levels(splits[5], (RESP, LEN), ((0, 32),), -0.2, 0.2), -12.5, -9.5)
    advantages = noise(splits[6], (RESP, LEN), 1.0, 4.0, ((0, 32),), jnp.float32)
    rollout_logp = draw_rollout_logp(jax.random.fold_in(splits[9], 71), 0)
    rollout_row = jax.random.permutation(splits[8], RESP).astype(jnp.int32)
    return {"hidden": hidden, "norm_gain": norm_gain, "head_weight": head_weight, "token_ids": token_ids, "lengths": lengths, "old_logp": old_logp, "advantages": advantages, "rollout_logp": rollout_logp, "rollout_row": rollout_row}


clip_eps = 0.2
kl_coef = 0.2
log_limit = 10.0
norm_eps = 1e-06

def token_terms(new_logp, old_logp, advantages, ref_logp, live_mask, prob_square):
    shift = new_logp - old_logp
    prob_ratio = jnp.exp(jnp.clip(shift, -log_limit, log_limit))
    clipped = jnp.clip(prob_ratio, 1.0 - clip_eps, 1.0 + clip_eps)
    plain_term = prob_ratio * advantages
    bounded_term = clipped * advantages
    surrogate = jnp.minimum(plain_term, bounded_term)
    ref_gap = ref_logp - new_logp
    gap_clip = jnp.clip(ref_gap, -log_limit, log_limit)
    kl_term = jnp.exp(gap_clip) - gap_clip - 1.0
    token_loss = live_mask * (kl_coef * kl_term - surrogate)
    inside_gap = (jnp.abs(ref_gap) < log_limit).astype(jnp.float32)
    inside_ratio = (jnp.abs(shift) < log_limit).astype(jnp.float32)
    active_term = (plain_term <= bounded_term).astype(jnp.float32)
    grad_coef = live_mask * (kl_coef * (1.0 - jnp.exp(gap_clip)) * inside_gap - advantages * prob_ratio * active_term * inside_ratio)
    grad_square = grad_coef * grad_coef * (prob_square - 2.0 * jnp.exp(new_logp) + 1.0)
    return (token_loss, live_mask * kl_term, grad_square)

def reference(hidden, norm_gain, head_weight, token_ids, lengths, old_logp, advantages, rollout_logp, rollout_row):
    values = hidden.astype(jnp.float32)
    inv_rms = lax.rsqrt(lax.optimization_barrier(jnp.mean(values * values, axis=1, keepdims=True)) + norm_eps)
    normed = (values * inv_rms * norm_gain.astype(jnp.float32)[None, :]).astype(jnp.bfloat16)
    blocks = normed.reshape(token_ids.shape[0], token_ids.shape[1], normed.shape[1])

    def per_response(block):
        block_rows, block_ids = block
        logits = jnp.dot(block_rows, head_weight, preferred_element_type=jnp.float32)
        row_max = lax.optimization_barrier(jnp.max(logits, axis=1))
        shifted = jnp.exp(logits - row_max[:, None])
        exp_sum = lax.optimization_barrier(jnp.sum(shifted, axis=1))
        exp_square = lax.optimization_barrier(jnp.sum(shifted * shifted, axis=1))
        picked = jnp.take_along_axis(logits, block_ids[:, None].astype(jnp.int32), axis=1)[:, 0]
        return (picked - row_max - jnp.log(exp_sum), exp_square / (exp_sum * exp_sum))
    new_logp, prob_square = lax.map(per_response, (blocks, token_ids))
    ref_logp = jnp.take(rollout_logp, rollout_row.astype(jnp.int32), axis=0)
    positions = lax.broadcasted_iota(jnp.int32, token_ids.shape, 1)
    live_mask = (positions < lengths[:, None]).astype(jnp.float32)
    token_loss, kl_part, grad_part = token_terms(new_logp, old_logp, advantages, ref_logp, live_mask, prob_square)
    live_count = jnp.sum(live_mask)
    summary = jnp.stack([jnp.sum(token_loss) / live_count, jnp.sum(kl_part) / live_count, jnp.sqrt(jnp.sum(grad_part) / live_count)])
    return (new_logp, token_loss, summary)
```

```python
import functools
import heapq

import jax
import jax.numpy as jnp
from jax import lax
from jax.experimental import pallas as pl
from jax.experimental.pallas import tpu as pltpu
from jax.sharding import PartitionSpec as P

clip_eps = 0.2
kl_coef = 0.2
log_limit = 10.0
norm_eps = 1e-06

MESH = pl.DeviceIdType.MESH
LOW = -1e30
CHUNK = 256
SUB = 128
STEP = 256
DEPTH = 3


def through_y(pair):
    return pair % 2 == 1


def links_of(item, subs):
    out = []
    if item[0] == "w":
        _, col, dy, pair, r = item
        if col == 0:
            if dy == 0 or (dy == 3 and r == 0):
                out.append("yp")
            if dy == 0 or (dy == 1 and r == 1):
                out.append("ym")
            if r == 1 and not (dy == 2 and through_y(pair)):
                out.append("h")
        else:
            if r == 0 and not (dy == 2 and through_y(pair)):
                out.append("l")
            if through_y(pair) and (dy, r) == (3, 0):
                out.append("yp")
            if through_y(pair) and (dy, r) == (1, 1):
                out.append("ym")
    else:
        _, dz, sub = item
        first = sub < subs // 2
        if dz in (0, 7, 6) or (dz == 5 and first):
            out.append("zp")
        if dz in (0, 1, 2) or (dz == 3 and not first):
            out.append("zm")
    return out


def arrives_as(link, item):
    if item[0] == "w":
        _, col, dy, pair, r = item
        if link == "yp":
            return ("w", col, (dy - 1) % 4, pair, r)
        if link == "ym":
            return ("w", col, (dy + 1) % 4, pair, r)
        if link == "h":
            return ("w", 1 - col, dy, pair, 1 - r)
        return ("w", col, dy, pair, 1 - r)
    return ("h", (item[1] + (-1 if link == "zp" else 1)) % 8, item[2])


def rank(link, item):
    if item[0] == "w":
        return (item[3], item[2] != 0 if link[0] == "y" else 0, item[1], item[4])
    return (min(item[1], 8 - item[1]) + item[2] / 4, item[2])


def plan(pairs, subs):
    wire = {"w": 2.85, "h": 1.45}
    delay, norm_time, chunk_time, own_time = 2.0, 0.8, 1.4, 2.0
    names = ("zp", "zm", "yp", "ym", "h", "l")
    free = dict.fromkeys(names, 0.0)
    ends = {n: [] for n in names}
    ready = {n: [] for n in names}
    arrivals, ops = [], []
    for sub in range(subs):
        heapq.heappush(arrivals, (0.0, ("h", 0, sub)))
    for pair in range(pairs):
        for r in (0, 1):
            heapq.heappush(arrivals, (own_time, ("w", 0, 0, pair, r)))
    missing = {("c", pair, r): 8 for pair in range(pairs) for r in (0, 1)}
    missing.update({("n", sub): 8 for sub in range(subs)})
    tokens_missing, normable, computable = 2 * subs, [], []
    now = 0.0

    def top_up():
        for n in names:
            ends[n] = [e for e in ends[n] if e > now]
            while ready[n] and len(ends[n]) < DEPTH:
                _, item = heapq.heappop(ready[n])
                end = max(now, free[n]) + wire[item[0]]
                free[n] = end
                ends[n].append(end)
                ops.append(("send", n, item))
                heapq.heappush(arrivals, (end + delay, arrives_as(n, item)))

    while arrivals or normable or computable:
        if arrivals and arrivals[0][0] <= now:
            _, item = heapq.heappop(arrivals)
            own = item[0] == "h" and item[1] == 0 or item[0] == "w" and item[1:3] == (0, 0)
            if not own or item[0] == "w" and item[3:] == (0, 0) or item == ("h", 0, 0):
                ops.append(("wait", item))
            if item[0] == "p":
                tokens_missing -= 1
                continue
            for n in links_of(item, subs):
                heapq.heappush(ready[n], (rank(n, item), item))
            if not own or not arrivals or arrivals[0][0] > now:
                top_up()
            key = ("c", *item[3:]) if item[0] == "w" else ("n", item[2])
            missing[key] -= 1
            if missing[key] == 0:
                (computable if key[0] == "c" else normable).append(key)
        elif normable:
            key = normable.pop(0)
            now += norm_time
            ops.append(("norm", key[1]))
            tokens_missing -= 1
            heapq.heappush(arrivals, (now + 1.8, ("p", key[1])))
            top_up()
        elif computable and tokens_missing == 0:
            key = computable.pop(0)
            now += chunk_time
            ops.append(("chunk", *key[1:]))
            top_up()
        else:
            now = max(now, arrivals[0][0])
            top_up()
    return ops, now


def kernel(
    hidden, gain, weight, ids, lens, old, adv, roll, row,
    logp_out, loss_out, sum_out,
    w_all, w_own, w_send, hid, normed, id_peer, id_cols, m_acc, s_acc, q_acc, p_acc,
    stat_rows, stat_peer, stat_all, ref_rows, ref_all, gains, tot_all,
    local_sem, w_sem, h_sem, n_sem, g_sem, r_sem, z_sem, s_sem, t_sem, pair_sem, send_sem,
):
    lo, f, z = lax.axis_index("dp"), lax.axis_index("fsdp"), lax.axis_index("tensor")
    hi, y, c = f // 8, (f // 2) % 4, f % 2
    me = lo * 16 + f
    subs = hid.shape[1] // SUB
    chunks = w_all.shape[0]
    rows_dev, cols = weight.shape
    half = chunks * CHUNK
    own_tokens = ids.shape[1]
    zs = stat_all.shape[0]
    blocks = own_tokens // 128

    def at(hi_, lo_, y_, c_, z_):
        return {"dp": lo_, "fsdp": hi_ * 8 + y_ * 2 + c_, "tensor": z_}

    partner = at(hi, lo, y, 1 - c, z)
    target = {
        "yp": at(hi, lo, (y + 1) % 4, c, z),
        "ym": at(hi, lo, (y + 3) % 4, c, z),
        "h": at(1 - hi, 1 - lo, y, c, z),
        "l": at(hi, 1 - lo, y, c, z),
        "zp": at(hi, lo, y, c, (z + 1) % zs),
        "zm": at(hi, lo, y, c, (z + zs - 1) % zs),
    }

    def plane_peer(k):
        other = (me + k) % 32
        return {"dp": other // 16, "fsdp": other % 16, "tensor": z}

    def line_peer(k):
        return {"dp": lo, "fsdp": f, "tensor": (z + k) % zs}

    def remote(src, dst, s, r, device):
        return pltpu.make_async_remote_copy(
            src_ref=src, dst_ref=dst, send_sem=s, recv_sem=r, device_id=device, device_id_type=MESH
        )

    hid_in = pltpu.make_async_copy(hidden, hid.at[z], local_sem.at[0])
    w_in = pltpu.make_async_copy(weight, w_own, local_sem.at[1])
    w_in.start()
    hid_in.start()

    barrier = pltpu.get_barrier_semaphore()

    @pl.loop(1, 32)
    def _(k):
        pl.semaphore_signal(barrier, inc=1, device_id=plane_peer(k), device_id_type=MESH)

    @pl.loop(1, zs)
    def _(k):
        pl.semaphore_signal(barrier, inc=1, device_id=line_peer(k), device_id_type=MESH)

    lane = lax.broadcasted_iota(jnp.int32, (1, 128), 1)
    group = hi * 4 + y
    row0 = pl.multiple_of(group * 256 + c * rows_dev, rows_dev)
    gains[z] = gain[...].astype(jnp.float32)
    own_roll = roll[...]
    ref_rows[me] = jnp.concatenate([own_roll, own_roll], axis=1)
    w_in.wait()

    def split(own):
        for side in (own, 1 - own):
            for j in range(chunks):
                start = side * half + j * CHUNK
                width = min(CHUNK, cols - start)
                if width < CHUNK:
                    if side == own:
                        w_all[j, pl.ds(row0, rows_dev), :] = jnp.zeros((rows_dev, CHUNK), jnp.bfloat16)
                    else:
                        w_send[j] = jnp.zeros((rows_dev, CHUNK), jnp.bfloat16)
                piece = w_own[:, start : start + width]
                if side == own:
                    w_all[j, pl.ds(row0, rows_dev), :width] = piece
                else:
                    w_send[j, :, :width] = piece

    @pl.when(c == 0)
    def _():
        split(0)

    @pl.when(c == 1)
    def _():
        split(1)

    hid_in.wait()
    pl.semaphore_wait(barrier, 31 + zs - 1)

    id_copy = remote(ids, id_peer, send_sem.at[0], pair_sem.at[0], partner)
    w_pair = remote(w_send, w_all.at[:, pl.ds(row0, rows_dev), :], send_sem.at[1], pair_sem.at[1], partner)

    def w_piece(col, dy, pair, r):
        g = (1 - hi if col else hi) * 4 + (y + dy) % 4
        j = 2 * pair + (1 - lo if r else lo)
        return w_all.at[j, pl.ds(pl.multiple_of(g * 256, 256), 256), :], w_sem.at[g, j]

    def h_piece(dz, sub):
        owner = (z + dz) % zs
        return hid.at[owner, pl.ds(sub * SUB, SUB), :], h_sem.at[owner, sub]

    def move(link, item):
        if item[0] == "w":
            ref, sem = w_piece(*item[1:])
            return remote(ref, ref, send_sem.at[2], sem, target[link])
        ref, sem = h_piece(*item[1:])
        return remote(ref, ref, send_sem.at[3], sem, target[link])

    def token_rows(core, sub):
        return normed.at[pl.ds(pl.multiple_of(core * own_tokens + sub * SUB, SUB), SUB), :]

    def normalize(sub):
        @pl.loop(0, SUB // 32)
        def _(t):
            rows = pl.ds(pl.multiple_of(sub * SUB + t * 32, 32), 32)
            squares = jnp.zeros((32, 1), jnp.float32)
            for k in range(zs):
                part = hid[k, rows, :].astype(jnp.float32)
                squares += jnp.sum(part * part, axis=1, keepdims=True)
            inv = lax.rsqrt(squares * (1.0 / (zs * hid.shape[2])) + norm_eps)
            out = pl.ds(pl.multiple_of(c * own_tokens + sub * SUB + t * 32, 32), 32)
            for k in range(zs):
                part = hid[k, rows, :].astype(jnp.float32)
                width = hid.shape[2]
                normed[out, k * width : (k + 1) * width] = (part * inv * gains[k]).astype(jnp.bfloat16)

    def pair_tokens(sub):
        ref = token_rows(c, sub)
        return remote(ref, ref, send_sem.at[4], n_sem.at[sub], partner)

    def chunk(j):
        base = c * half + j * CHUNK

        @pl.loop(0, normed.shape[0] // STEP)
        def _(t):
            rows = pl.ds(pl.multiple_of(t * STEP, STEP), STEP)
            logits = jnp.dot(normed[rows, :], w_all[j], preferred_element_type=jnp.float32)
            col_a = base + lax.broadcasted_iota(jnp.int32, (STEP, 128), 1)
            wanted = id_cols[rows, :]
            a = jnp.where(col_a < cols, logits[:, :128], LOW)
            b = jnp.where(col_a < cols - 128, logits[:, 128:], LOW)
            where = wanted - col_a.astype(jnp.float32)
            p_acc[rows, :] += jnp.where(where == 0.0, a, 0.0) + jnp.where(where == 128.0, b, 0.0)
            old_max = m_acc[rows, :]
            new_max = jnp.maximum(old_max, jnp.maximum(a, b))
            scale = jnp.exp(old_max - new_max)
            exp_a, exp_b = jnp.exp(a - new_max), jnp.exp(b - new_max)
            s_acc[rows, :] = s_acc[rows, :] * scale + (exp_a + exp_b)
            q_acc[rows, :] = q_acc[rows, :] * (scale * scale) + (exp_a * exp_a + exp_b * exp_b)
            m_acc[rows, :] = new_max

    def ref_start():
        @pl.loop(1, 32)
        def _(k):
            remote(ref_rows.at[me], ref_rows.at[me], send_sem.at[5], r_sem.at[k], plane_peer(k)).start()

    def ref_pick():
        @pl.loop(1, 32)
        def _(k):
            src = ref_rows.at[(me + 32 - k) % 32]
            remote(src, src, send_sem.at[5], r_sem.at[k], partner).wait_recv()

        ref_all[z] = ref_rows[row[0]]

    def ref_send():
        @pl.loop(1, zs)
        def _(k):
            remote(ref_all.at[z], ref_all.at[z], send_sem.at[6], z_sem.at[k], line_peer(k)).start()

    def ref_wait():
        @pl.loop(1, zs)
        def _(k):
            src = ref_all.at[(z + zs - k) % zs]
            remote(src, src, send_sem.at[6], z_sem.at[k], partner).wait_recv()

    def ids_to_columns():
        remote(ids, id_peer, send_sem.at[0], pair_sem.at[0], partner).wait_recv()
        for b in range(2 * blocks):
            source = ids if b < blocks else id_peer
            line = source[:, (b % blocks) * 128 : (b % blocks + 1) * 128] - z * cols
            line = jnp.where((line >= 0) & (line < cols), line, -chunks * CHUNK * 4).astype(jnp.float32)
            core = c if b < blocks else 1 - c
            out = pl.ds(pl.multiple_of(core * own_tokens + (b % blocks) * 128, 128), 128)
            id_cols[out, :] = jnp.transpose(jnp.broadcast_to(line, (128, 128)))

    def clear():
        m_acc[...] = jnp.full(m_acc.shape, LOW, jnp.float32)
        s_acc[...] = jnp.zeros(s_acc.shape, jnp.float32)
        q_acc[...] = jnp.zeros(q_acc.shape, jnp.float32)
        p_acc[...] = jnp.zeros(p_acc.shape, jnp.float32)

    w_pair.start()
    id_copy.start()

    @pl.loop(1, zs)
    def _(k):
        remote(gains.at[z], gains.at[z], send_sem.at[7], g_sem.at[k], line_peer(k)).start()

    ops, _ = plan(chunks // 2, subs)
    extra = {0: ref_start, 24: clear, 26: ids_to_columns, 60: ref_pick, 64: ref_send, 110: ref_wait}
    gains_here = False
    for number, op in enumerate(ops):
        if op[0] == "send":
            move(op[1], op[2]).start()
        elif op[0] == "wait":
            item = op[1]
            if item[0] == "p":
                ref = token_rows(1 - c, item[1])
                remote(ref, ref, send_sem.at[4], n_sem.at[item[1]], partner).wait_recv()
            elif item[0] == "w" and item[1:3] == (0, 0):
                w_pair.wait_recv()
            elif item[0] == "w":
                ref, sem = w_piece(*item[1:])
                remote(ref, ref, send_sem.at[2], sem, partner).wait_recv()
            elif item[1] != 0:
                ref, sem = h_piece(*item[1:])
                remote(ref, ref, send_sem.at[3], sem, partner).wait_recv()
        elif op[0] == "norm":
            if not gains_here:
                gains_here = True

                @pl.loop(1, zs)
                def _(k):
                    src = gains.at[(z + zs - k) % zs]
                    remote(src, src, send_sem.at[7], g_sem.at[k], partner).wait_recv()

            normalize(op[1])
            pair_tokens(op[1]).start()
        else:
            chunk(2 * op[1] + (1 - lo if op[2] else lo))
        if number in extra:
            extra[number]()

    stat_rows[...] = jnp.zeros(stat_rows.shape, jnp.float32)

    def reduce_block(b, _):
        rows = pl.ds(pl.multiple_of(b * 128, 128), 128)
        lane_max = m_acc[rows, :]
        top = jnp.max(lane_max, axis=1, keepdims=True)
        scale = jnp.exp(lane_max - top)
        total = jnp.sum(s_acc[rows, :] * scale, axis=1, keepdims=True)
        square = jnp.sum(q_acc[rows, :] * (scale * scale), axis=1, keepdims=True)
        chosen = jnp.sum(p_acc[rows, :], axis=1, keepdims=True)
        place = jnp.where(b // blocks == c, 0, 16) + b % blocks
        spread = stat_rows[...]
        for k, value in enumerate((top, total, square, chosen)):
            spread = jnp.where(lane == place + k * blocks, value, spread)
        stat_rows[...] = spread
        return 0

    lax.fori_loop(0, 2 * blocks, reduce_block, 0)
    turned = jnp.transpose(stat_rows[...])
    stat_rows[...] = turned
    give = remote(stat_rows.at[pl.ds(16, 16)], stat_peer, send_sem.at[8], pair_sem.at[2], partner)
    give.start()
    give.wait_recv()

    def merge(parts):
        top = functools.reduce(jnp.maximum, [p[0:4] for p in parts])
        total = square = chosen = 0.0
        for p in parts:
            scale = jnp.exp(p[0:4] - top)
            total += p[4:8] * scale
            square += p[8:12] * (scale * scale)
            chosen += p[12:16]
        return top, total, square, chosen

    stat_all[z] = jnp.concatenate(merge([stat_rows[0:16, :], stat_peer[...]]), axis=0)

    @pl.loop(1, zs)
    def _(k):
        remote(stat_all.at[z], stat_all.at[z], send_sem.at[9], s_sem.at[k], line_peer(k)).start()

    @pl.loop(1, zs)
    def _(k):
        src = stat_all.at[(z + zs - k) % zs]
        remote(src, src, send_sem.at[9], s_sem.at[k], partner).wait_recv()

    top, total, square, chosen = merge([stat_all[k] for k in range(zs)])
    new_logp = chosen - top - jnp.log(total)
    prob_square = square / (total * total)

    def lines(ref):
        return jnp.concatenate([ref[:, b * 128 : (b + 1) * 128] for b in range(blocks)], axis=0)

    old_logp, advantages = lines(old), lines(adv)
    ref_logp = jnp.concatenate(
        [jnp.where(lane < 64, ref_all[2 * b], ref_all[2 * b + 1]) for b in range(blocks)], axis=0
    )
    position = lax.broadcasted_iota(jnp.int32, (blocks, 128), 0) * 128 + lax.broadcasted_iota(
        jnp.int32, (blocks, 128), 1
    )
    live = jnp.where(position < lens[0], 1.0, 0.0)
    shift = new_logp - old_logp
    prob_ratio = jnp.exp(jnp.clip(shift, -log_limit, log_limit))
    clipped = jnp.clip(prob_ratio, 1.0 - clip_eps, 1.0 + clip_eps)
    plain_term = prob_ratio * advantages
    bounded_term = clipped * advantages
    surrogate = jnp.minimum(plain_term, bounded_term)
    ref_gap = ref_logp - new_logp
    gap_clip = jnp.clip(ref_gap, -log_limit, log_limit)
    gap_exp = jnp.exp(gap_clip)
    kl_term = gap_exp - gap_clip - 1.0
    token_loss = live * (kl_coef * kl_term - surrogate)
    inside_gap = jnp.where(jnp.abs(ref_gap) < log_limit, 1.0, 0.0)
    inside_ratio = jnp.where(jnp.abs(shift) < log_limit, 1.0, 0.0)
    active = jnp.where(plain_term <= bounded_term, 1.0, 0.0)
    grad = live * (kl_coef * (1.0 - gap_exp) * inside_gap - advantages * prob_ratio * active * inside_ratio)
    grad_square = grad * grad * (prob_square - 2.0 * jnp.exp(new_logp) + 1.0)

    def whole(array):
        return jnp.sum(jnp.sum(array, axis=0, keepdims=True), axis=1, keepdims=True)

    own_sums = jnp.zeros((1, 128), jnp.float32)
    for k, value in enumerate((live, token_loss, live * kl_term, grad_square)):
        own_sums = jnp.where(lane == k, whole(value), own_sums)
    tot_all[me] = own_sums

    @pl.loop(1, 32)
    def _(k):
        remote(tot_all.at[me], tot_all.at[me], send_sem.at[10], t_sem.at[k], plane_peer(k)).start()

    for b in range(blocks):
        logp_out[:, b * 128 : (b + 1) * 128] = new_logp[b : b + 1, :]
        loss_out[:, b * 128 : (b + 1) * 128] = token_loss[b : b + 1, :]

    @pl.loop(1, 32)
    def _(k):
        src = tot_all.at[(me + 32 - k) % 32]
        remote(src, src, send_sem.at[10], t_sem.at[k], partner).wait_recv()

    sums = functools.reduce(jnp.add, [tot_all[k] for k in range(32)])
    count, loss, kl, grads = [
        jnp.sum(jnp.where(lane == k, sums, 0.0), axis=1, keepdims=True) for k in range(4)
    ]
    sum_out[...] = jnp.where(
        lane == 0, loss / count, jnp.where(lane == 1, kl / count, jnp.sqrt(grads / count))
    )

    def left(src, k):
        remote(src, src, send_sem.at[k], local_sem.at[0], partner).wait_send()

    left(ids, 0)
    left(w_send, 1)
    left(w_all.at[:, 0 : 7 * 256, :], 2)
    left(hid.at[0 : zs - 1], 3)
    left(normed.at[0:own_tokens, :], 4)
    left(ref_rows.at[0:31], 5)
    left(ref_all.at[0 : zs - 1], 6)
    left(gains.at[0 : zs - 1], 7)
    left(stat_peer, 8)
    left(stat_all.at[0 : zs - 1], 9)
    left(tot_all.at[0:31], 10)


def shards(hidden, norm_gain, head_weight, token_ids, lengths, old_logp, advantages, rollout_logp, rollout_row):
    tokens, features = hidden.shape
    rows_dev, cols = head_weight.shape
    zs = lax.axis_size("tensor")
    depth = features * zs
    chunks = 8
    vmem = pl.BlockSpec(memory_space=pltpu.VMEM)
    smem = pl.BlockSpec(memory_space=pltpu.SMEM)
    anywhere = pl.BlockSpec(memory_space=pl.ANY)
    f32, bf16 = jnp.float32, jnp.bfloat16
    dma = pltpu.SemaphoreType.DMA
    new_logp, token_loss, summary = pl.pallas_call(
        kernel,
        out_shape=(
            jax.ShapeDtypeStruct((1, tokens), f32),
            jax.ShapeDtypeStruct((1, tokens), f32),
            jax.ShapeDtypeStruct((1, 128), f32),
        ),
        in_specs=[anywhere, vmem, anywhere, vmem, smem, vmem, vmem, vmem, smem],
        out_specs=(vmem, vmem, vmem),
        scratch_shapes=[
            pltpu.VMEM((chunks, depth, CHUNK), bf16),
            pltpu.VMEM((rows_dev, cols), bf16),
            pltpu.VMEM((chunks, rows_dev, CHUNK), bf16),
            pltpu.VMEM((zs, tokens, features), bf16),
            pltpu.VMEM((2 * tokens, depth), bf16),
            pltpu.VMEM((1, tokens), jnp.int32),
            pltpu.VMEM((2 * tokens, 128), f32),
            pltpu.VMEM((2 * tokens, 128), f32),
            pltpu.VMEM((2 * tokens, 128), f32),
            pltpu.VMEM((2 * tokens, 128), f32),
            pltpu.VMEM((2 * tokens, 128), f32),
            pltpu.VMEM((128, 128), f32),
            pltpu.VMEM((16, 128), f32),
            pltpu.VMEM((zs, 16, 128), f32),
            pltpu.VMEM((32, 1, 128), f32),
            pltpu.VMEM((zs, 1, 128), f32),
            pltpu.VMEM((zs, 1, features), f32),
            pltpu.VMEM((32, 1, 128), f32),
            dma((2,)),
            dma((8, chunks)),
            dma((zs, tokens // SUB)),
            dma((tokens // SUB,)),
            dma((zs,)),
            dma((32,)),
            dma((zs,)),
            dma((zs,)),
            dma((32,)),
            dma((3,)),
            dma((11,)),
        ],
        compiler_params=pltpu.CompilerParams(
            collective_id=0, has_side_effects=True, vmem_limit_bytes=48 * 1024 * 1024
        ),
    )(
        hidden, norm_gain.reshape(1, features), head_weight, token_ids, lengths, old_logp, advantages, rollout_logp,
        rollout_row,
    )
    return new_logp, token_loss, summary[0, :3]


def solution(mesh):
    in_specs = (
        P(("dp", "fsdp"), "tensor"),
        P("tensor"),
        P("fsdp", "tensor"),
        P(("dp", "fsdp"), None),
        P(("dp", "fsdp")),
        P(("dp", "fsdp"), None),
        P(("dp", "fsdp"), None),
        P(("dp", "fsdp"), "tensor"),
        P(("dp", "fsdp")),
    )
    out_specs = (P(("dp", "fsdp"), None), P(("dp", "fsdp"), None), P())
    return jax.shard_map(shards, mesh=mesh, in_specs=in_specs, out_specs=out_specs, check_vma=False)
```

```python
import collections
import functools
import heapq

import jax
import jax.numpy as jnp
from jax import lax
from jax.experimental import pallas as pl
from jax.experimental.pallas import tpu as pltpu
from jax.sharding import PartitionSpec as P

clip_eps = 0.2
kl_coef = 0.2
log_limit = 10.0
norm_eps = 1e-06

MESH = pl.DeviceIdType.MESH
LOW = -1e30
CHUNK = 256
SUB = 128
DEPTH = 2
BATCH = 4
CHUNKS = 4
SUBS = 4
NEAR = (0, 1, 3, 6, 7)
TUNE = dict(y_far=-0.23, y_col=0.99, h_dy=(14.71, 7.92, -16.21, 18.43), z_hop=-74.15, z_sub=-20.38, z_late=-48.75, l_hop=-29.58, l_sub=22.48, by_h=())


def way_in(item):
    if item[0] == "w":
        _, col, dy, j = item
        if col == 0:
            if dy == 2:
                return "yp" if j < CHUNKS // 2 else "ym"
            return {0: None, 3: "yp", 1: "ym"}[dy]
        if dy in (0, 2) or j in TUNE["by_h"]:
            return "h"
        return "yp" if dy == 3 else "ym"
    _, who, dz, sub = item
    if who == 0 and dz == 0:
        return None
    if who == 1 and dz in NEAR:
        return "l"
    if dz == 4:
        return "zp" if sub < SUBS // 2 else "zm"
    return "zp" if dz > 4 else "zm"


def arrives_as(link, item):
    if item[0] == "w":
        _, col, dy, j = item
        if link == "h":
            return ("w", 1 - col, dy, j)
        return ("w", col, (dy + (3 if link == "yp" else 1)) % 4, j)
    _, who, dz, sub = item
    if link == "l":
        return ("h", 1 - who, dz, sub)
    return ("h", who, (dz + (7 if link == "zp" else 1)) % 8, sub)


def links_of(item):
    names = ("yp", "ym", "h") if item[0] == "w" else ("zp", "zm", "l")
    return [n for n in names if way_in(arrives_as(n, item)) == n]


def rank(link, item):
    t = TUNE
    if item[0] == "w":
        _, col, dy, j = item
        if link == "h":
            return (j + t["h_dy"][dy], dy)
        return (j + (t["y_far"] if dy else 0.0) + t["y_col"] * col, dy)
    _, who, dz, sub = item
    hops = min(dz, 8 - dz)
    if link == "l":
        return (hops * t["l_hop"] + sub * t["l_sub"], dz)
    return (hops * t["z_hop"] + sub * t["z_sub"] + who * t["z_late"], dz)


def plan():
    wire = {"w": 2.85, "h": 1.43}
    delay = 2.0
    norm_time, jobs_time, unit_time = 0.45, 0.15, 0.4
    names = ("zp", "zm", "l", "yp", "ym", "h")
    free = dict.fromkeys(names, 0.0)
    ends = {n: [] for n in names}
    ready = {n: [] for n in names}
    arrivals, ops = [], []
    for sub in range(SUBS):
        heapq.heappush(arrivals, (0.0, ("h", 0, 0, sub)))
    for j in range(CHUNKS):
        heapq.heappush(arrivals, (1.0 + 0.2 * j, ("w", 0, 0, j)))
    tokens = [(who, sub) for sub in range(SUBS) for who in (0, 1)]
    missing = {("c", j): 8 for j in range(CHUNKS)}
    missing.update({("n", *w): 8 for w in tokens})
    token_parts = {w: 2 for w in tokens}
    norms, units, chunks_here, tokens_here = [], [], [], []
    now = 0.0

    def top_up():
        for n in names:
            ends[n] = [e for e in ends[n] if e > now]
            while ready[n] and len(ends[n]) < DEPTH:
                _, item = heapq.heappop(ready[n])
                end = max(now, free[n]) + wire[item[0]]
                free[n] = end
                ends[n].append(end)
                ops.append(("send", n, item))
                heapq.heappush(arrivals, (end + delay, arrives_as(n, item)))

    def part_of(w):
        token_parts[w] -= 1
        if token_parts[w] == 0:
            tokens_here.append(w)
            units.extend((*w, j) for j in chunks_here)

    while arrivals or norms or units:
        if arrivals and arrivals[0][0] <= now:
            _, item = heapq.heappop(arrivals)
            ops.append(("wait", item))
            if item[0] == "p":
                part_of(item[1:])
                continue
            for n in links_of(item):
                heapq.heappush(ready[n], (rank(n, item), item))
            if not arrivals or arrivals[0][0] > now:
                top_up()
            key = ("c", item[3]) if item[0] == "w" else ("n", item[1], item[3])
            missing[key] -= 1
            if missing[key] == 0:
                if key[0] == "c":
                    chunks_here.append(key[1])
                    units.extend((*w, key[1]) for w in tokens_here)
                else:
                    norms.append(key[1:])
        elif norms:
            who_sub = norms.pop(0)
            now += norm_time
            ops.append(("norm", who_sub))
            heapq.heappush(arrivals, (now + 1.8, ("p", *who_sub)))
            part_of(who_sub)
            top_up()
        elif units:
            batch = sorted(units[:BATCH])
            del units[:BATCH]
            now += jobs_time + unit_time * len(batch)
            ops.append(("jobs", tuple(batch)))
            top_up()
        else:
            now = arrivals[0][0]
            top_up()
    return ops, now


def kernel(
    hidden, gain_in, weight, ids_in, lens, old_in, adv_in, roll_in, row,
    logp_out, loss_out, sum_out,
    w_all, hid, normed, ids, id_row, m_acc, s_acc, q_acc, p_acc,
    stat_rows, stat_quad, stat_all, ref_rows, ref_all, gains, tot_all, gain, old, adv, roll,
    local_sem, own_sem, wp_sem, w_sem, h_sem, n_sem, g_sem, all_sem, send_sem,
):
    lo, f, z = lax.axis_index("dp"), lax.axis_index("fsdp"), lax.axis_index("tensor")
    hi, y, c = f // 8, (f // 2) % 4, f % 2
    me = lo * 16 + f
    side = (lo + hi) % 2
    quarter = 2 * side + c
    cols, rows_dev = weight.shape
    zs, features = stat_all.shape[0], hid.shape[2]
    blocks = ids_in.shape[1] // 128
    last = cols - (4 * CHUNKS - 1) * CHUNK
    group = hi * 4 + y

    def at(hi_, lo_, y_, c_, z_):
        return {"dp": lo_, "fsdp": hi_ * 8 + y_ * 2 + c_, "tensor": z_}

    quad = [None, at(hi, lo, y, 1 - c, z), at(hi, 1 - lo, y, c, z), at(hi, 1 - lo, y, 1 - c, z)]
    partner = quad[1]
    target = {
        "yp": at(hi, lo, (y + 1) % 4, c, z),
        "ym": at(hi, lo, (y + 3) % 4, c, z),
        "h": at(1 - hi, 1 - lo, y, c, z),
        "l": quad[2],
        "zp": at(hi, lo, y, c, (z + 1) % zs),
        "zm": at(hi, lo, y, c, (z + zs - 1) % zs),
    }

    def plane_peer(k):
        other = (me + k) % 32
        return {"dp": other // 16, "fsdp": other % 16, "tensor": z}

    def line_peer(k):
        return {"dp": lo, "fsdp": f, "tensor": (z + k) % zs}

    def remote(src, dst, s, r, device):
        return pltpu.make_async_remote_copy(
            src_ref=src, dst_ref=dst, send_sem=s, recv_sem=r, device_id=device, device_id_type=MESH
        )

    def received(dst, r):
        remote(dst, dst, send_sem.at[0], r, partner).wait_recv()

    barrier = pltpu.get_barrier_semaphore()
    for device in (*quad[1:], *(target[n] for n in ("yp", "ym", "h", "zp", "zm"))):
        pl.semaphore_signal(barrier, inc=1, device_id=device, device_id_type=MESH)

    lane0 = pl.multiple_of(group * 256 + c * rows_dev, 128)

    def sized(j, owner, act):
        if j < CHUNKS - 1:
            act(CHUNK)
            return

        @pl.when(owner < 3)
        def _():
            act(CHUNK)

        @pl.when(owner == 3)
        def _():
            act(last)

    def own_weights(j, count):
        src = weight.at[pl.ds(pl.multiple_of((quarter * CHUNKS + j) * CHUNK, CHUNK), count), :]
        return pltpu.make_async_copy(src, w_all.at[j, pl.ds(0, count), pl.ds(lane0, 128)], own_sem.at[j])

    def pair_weights(j, count, owner):
        src = weight.at[pl.ds(pl.multiple_of((owner * CHUNKS + j) * CHUNK, CHUNK), count), :]
        dst = w_all.at[j, pl.ds(0, count), pl.ds(lane0, 128)]
        return remote(src, dst, send_sem.at[12 if j < CHUNKS - 1 else 0], wp_sem.at[j], partner)

    small = [
        pltpu.make_async_copy(src, dst, local_sem.at[k])
        for k, (src, dst) in enumerate(
            ((gain_in, gain), (roll_in, roll), (ids_in, ids.at[0]), (old_in, old), (adv_in, adv))
        )
    ]
    hid_in = pltpu.make_async_copy(hidden, hid.at[z], local_sem.at[5])
    hid_in.start()
    small[0].start()
    small[2].start()
    for j in range(CHUNKS):
        sized(j, quarter, lambda n, j=j: own_weights(j, n).start())
    for k in (1, 3, 4):
        small[k].start()

    @pl.when(quarter == 3)
    def _():
        pad = jnp.zeros((CHUNK - last, 256), jnp.bfloat16)
        w_all[CHUNKS - 1, last:CHUNK, pl.ds(pl.multiple_of(group * 256, 256), 256)] = pad

    lane = lax.broadcasted_iota(jnp.int32, (1, 128), 1)
    m_acc[...] = jnp.full(m_acc.shape, LOW, jnp.float32)
    s_acc[...] = jnp.zeros(s_acc.shape, jnp.float32)
    q_acc[...] = jnp.zeros(q_acc.shape, jnp.float32)
    p_acc[...] = jnp.zeros(p_acc.shape, jnp.float32)
    small[0].wait()
    gains[z] = gain[...].astype(jnp.float32).reshape(1, features)
    small[1].wait()
    ref_rows[0] = jnp.concatenate([roll[...], roll[...]], axis=1)
    small[2].wait()
    pl.semaphore_wait(barrier, 8)

    ops = plan()[0]
    first_who, first_sub = next(op[1] for op in ops if op[0] == "norm")
    assert first_who == 0

    def w_piece(col, dy, j):
        g = (1 - hi if col else hi) * 4 + (y + dy) % 4
        return w_all.at[j, :, pl.ds(pl.multiple_of(g * 256, 256), 256)], w_sem.at[g, j]

    def h_piece(who, dz, sub):
        owner = who * zs + (z + dz) % zs
        return hid.at[owner, pl.ds(sub * SUB, SUB), :], h_sem.at[owner, sub]

    def with_gain(link, item):
        return link[0] == "z" and item[1] == 0 and item[3] == first_sub

    def send(link, item):
        if item[0] == "w":
            ref, sem = w_piece(*item[1:])
            remote(ref, ref, send_sem.at[1], sem, target[link]).start()
            return
        ref, sem = h_piece(*item[1:])
        other = h_piece(1 - item[1], *item[2:]) if link == "l" else (ref, sem)
        remote(ref, other[0], send_sem.at[2 if link == "l" else 3], other[1], target[link]).start()
        if with_gain(link, item):
            k = (z + item[2]) % zs
            remote(gains.at[k], gains.at[k], send_sem.at[4], g_sem.at[k], target[link]).start()

    def place(who, sub, core):
        return pl.multiple_of(((who * SUBS + sub) * 2 + core) * SUB, SUB)

    def wait(item):
        if item[0] == "p":
            received(normed.at[pl.ds(place(*item[1:], 1 - c), SUB), :], n_sem.at[item[1], item[2]])
        elif item[0] == "w" and item[1:3] == (0, 0):
            j = item[3]
            sized(j, quarter, lambda n: own_weights(j, n).wait())
            sized(j, quarter, lambda n: received(w_all.at[j, pl.ds(0, n), pl.ds(lane0, 128)], wp_sem.at[j]))
        elif item[0] == "w":
            received(*w_piece(*item[1:]))
        elif item[1:3] != (0, 0):
            received(*h_piece(*item[1:]))
            if item[1] == 0 and item[3] == first_sub:
                k = (z + item[2]) % zs
                received(gains.at[k], g_sem.at[k])

    def normalize(who, sub):
        gain_rows = [gains[k] for k in range(zs)]
        for t in range(0, SUB, 32):
            rows = slice(sub * SUB + t, sub * SUB + t + 32)
            squares = jnp.zeros((32, features), jnp.float32)
            for k in range(zs):
                part = hid[who * zs + k, rows, :].astype(jnp.float32)
                squares += part * part
            mean = jnp.sum(squares, axis=1, keepdims=True) * (1.0 / (zs * features))
            inv = lax.rsqrt(mean + norm_eps)
            out = pl.ds(pl.multiple_of(place(who, sub, c) + t, 32), 32)
            for k in range(zs):
                part = hid[who * zs + k, rows, :].astype(jnp.float32)
                normed[out, k * features : (k + 1) * features] = (part * inv * gain_rows[k]).astype(jnp.bfloat16)

        ref = normed.at[pl.ds(place(who, sub, c), SUB), :]
        remote(ref, ref, send_sem.at[5], n_sem.at[who, sub], partner).start()

    def job(who, sub, j):
        base = (quarter * CHUNKS + j) * CHUNK
        start = (who * SUBS + sub) * 2 * SUB
        tokens = slice(start, start + 2 * SUB)
        logits = lax.dot_general(
            w_all[j], normed[tokens, :], (((1,), (1,)), ((), ())), preferred_element_type=jnp.float32
        ).reshape(CHUNK // 8, 8, 2 * SUB)
        shape = (CHUNK // 8, 8, 1)
        column = lax.broadcasted_iota(jnp.int32, shape, 0) * 8 + lax.broadcasted_iota(jnp.int32, shape, 1)
        if j == CHUNKS - 1:
            logits = jnp.where(column < cols - base, logits, LOW)
        wanted = (id_row[:, tokens] - base)[None]
        p_acc[:, tokens] += jnp.sum(jnp.where(column == wanted, logits, 0.0), axis=0)
        old_max = m_acc[:, tokens]
        new_max = jnp.maximum(old_max, jnp.max(logits, axis=0))
        scale = jnp.exp(old_max - new_max)
        exps = jnp.exp(logits - new_max[None])
        s_acc[:, tokens] = s_acc[:, tokens] * scale + jnp.sum(exps, axis=0)
        q_acc[:, tokens] = q_acc[:, tokens] * (scale * scale) + jnp.sum(exps * exps, axis=0)
        m_acc[:, tokens] = new_max

    def ids_to_row():
        received(ids.at[1:4], all_sem.at[0])
        for s in range(4):
            for sub in range(SUBS):
                line = ids[s, :, sub * 128 : (sub + 1) * 128] - z * cols
                line = jnp.where((line >= 0) & (line < cols), line, -(1 << 20))
                id_row[:, pl.ds(place(s // 2, sub, (c + s) % 2), 128)] = line

    def to_plane(array, s, r):
        @pl.loop(0, 31)
        def _(i):
            k = (i + 15) % 31 + 1
            remote(array.at[0], array.at[k], send_sem.at[s], all_sem.at[r], plane_peer(k)).start()

    def to_line(array, s, r):
        for k in (4, 3, 5, 2, 6, 1, 7):
            remote(array.at[0], array.at[k], send_sem.at[s], all_sem.at[r], line_peer(k)).start()

    def all_received(array, r):
        received(array.at[1:], all_sem.at[r])

    def ref_start():
        to_plane(ref_rows, 6, 1)

    def ref_pick():
        all_received(ref_rows, 1)
        ref_all[0] = ref_rows[(me + 32 - row[0]) % 32]

    def ref_send():
        to_line(ref_all, 7, 2)

    def ref_wait():
        all_received(ref_all, 2)

    other = 2 * side + 1 - c
    for j in range(CHUNKS):
        sized(j, other, lambda n, j=j: pair_weights(j, n, other).start())
    for s in range(1, 4):
        remote(ids.at[0], ids.at[s], send_sem.at[8], all_sem.at[0], quad[s]).start()
    hid_in.wait()

    batches = 0
    extra = {1: ref_start, 4: ref_pick, 5: ref_send, 8: ref_wait}
    for number, op in enumerate(ops):
        if op[0] == "send":
            send(op[1], op[2])
        elif op[0] == "wait":
            wait(op[1])
        elif op[0] == "norm":
            normalize(*op[1])
        else:
            for unit in op[1]:
                job(*unit)
            batches += 1
            if batches in extra:
                extra[batches]()
        if number == 40:
            ids_to_row()

    top = jnp.max(m_acc[...], axis=0, keepdims=True)
    scale = jnp.exp(m_acc[...] - top)
    total = jnp.sum(s_acc[...] * scale, axis=0, keepdims=True)
    square = jnp.sum(q_acc[...] * (scale * scale), axis=0, keepdims=True)
    chosen = jnp.sum(p_acc[...], axis=0, keepdims=True)
    for who in (0, 1):
        for core in (0, 1):
            starts = [((who * SUBS + sub) * 2 + core) * SUB for sub in range(SUBS)]
            stat_rows[who * 2 + (core + c) % 2] = jnp.concatenate(
                [value[:, i : i + SUB] for value in (top, total, square, chosen) for i in starts], axis=0
            )
    for s in range(1, 4):
        remote(stat_rows.at[s], stat_quad.at[s - 1], send_sem.at[9], all_sem.at[3], quad[s]).start()
    received(stat_quad, all_sem.at[3])

    def merge(parts):
        top = functools.reduce(jnp.maximum, [p[0:4] for p in parts])
        total = square = chosen = 0.0
        for p in parts:
            scale = jnp.exp(p[0:4] - top)
            total += p[4:8] * scale
            square += p[8:12] * (scale * scale)
            chosen += p[12:16]
        return top, total, square, chosen

    stat_all[0] = jnp.concatenate(merge([stat_rows[0], *(stat_quad[s] for s in range(3))]), axis=0)

    to_line(stat_all, 10, 4)
    small[3].wait()
    small[4].wait()
    all_received(stat_all, 4)

    top, total, square, chosen = merge([stat_all[k] for k in range(zs)])
    new_logp = chosen - top - jnp.log(total)
    prob_square = square / (total * total)

    def lines(ref):
        return jnp.concatenate([ref[:, b * 128 : (b + 1) * 128] for b in range(blocks)], axis=0)

    old_logp, advantages = lines(old), lines(adv)
    ref_logp = jnp.concatenate(
        [jnp.where(lane < 64, ref_all[(z + zs - 2 * b) % zs], ref_all[(z + zs - 2 * b - 1) % zs]) for b in range(blocks)], axis=0
    )
    position = lax.broadcasted_iota(jnp.int32, (blocks, 128), 0) * 128 + lax.broadcasted_iota(
        jnp.int32, (blocks, 128), 1
    )
    live = jnp.where(position < lens[0], 1.0, 0.0)
    shift = new_logp - old_logp
    prob_ratio = jnp.exp(jnp.clip(shift, -log_limit, log_limit))
    clipped = jnp.clip(prob_ratio, 1.0 - clip_eps, 1.0 + clip_eps)
    plain_term = prob_ratio * advantages
    bounded_term = clipped * advantages
    surrogate = jnp.minimum(plain_term, bounded_term)
    ref_gap = ref_logp - new_logp
    gap_clip = jnp.clip(ref_gap, -log_limit, log_limit)
    gap_exp = jnp.exp(gap_clip)
    kl_term = gap_exp - gap_clip - 1.0
    token_loss = live * (kl_coef * kl_term - surrogate)
    inside_gap = jnp.where(jnp.abs(ref_gap) < log_limit, 1.0, 0.0)
    inside_ratio = jnp.where(jnp.abs(shift) < log_limit, 1.0, 0.0)
    active = jnp.where(plain_term <= bounded_term, 1.0, 0.0)
    grad = live * (kl_coef * (1.0 - gap_exp) * inside_gap - advantages * prob_ratio * active * inside_ratio)
    grad_square = grad * grad * (prob_square - 2.0 * jnp.exp(new_logp) + 1.0)

    def whole(array):
        return jnp.sum(jnp.sum(array, axis=0, keepdims=True), axis=1, keepdims=True)

    own_sums = jnp.zeros((1, 128), jnp.float32)
    for k, value in enumerate((live, token_loss, live * kl_term, grad_square)):
        own_sums = jnp.where(lane == k, whole(value), own_sums)
    tot_all[0] = own_sums

    to_plane(tot_all, 11, 5)

    for b in range(blocks):
        logp_out[:, b * 128 : (b + 1) * 128] = new_logp[b : b + 1, :]
        loss_out[:, b * 128 : (b + 1) * 128] = token_loss[b : b + 1, :]

    def left(src, sem):
        remote(src, src, sem, local_sem.at[0], partner).wait_send()

    left(weight.at[pl.ds(0, (CHUNKS - 1) * CHUNK), :], send_sem.at[12])
    sized(CHUNKS - 1, other, lambda n: left(weight.at[pl.ds(0, n), :], send_sem.at[0]))
    count = collections.Counter(
        op[1] if op[1] in ("l", "zp", "zm") else "w" for op in ops if op[0] == "send"
    )
    count["g"] = sum(op[0] == "send" and with_gain(op[1], op[2]) for op in ops)
    left(w_all.at[:, :, 0 : count["w"] // CHUNKS * 256], send_sem.at[1])
    left(hid.at[0 : count["l"] // SUBS], send_sem.at[2])
    left(hid.at[0 : (count["zp"] + count["zm"]) // SUBS], send_sem.at[3])
    left(gains.at[0 : count["g"]], send_sem.at[4])
    left(normed.at[0 : 2 * SUBS * SUB, :], send_sem.at[5])
    left(ref_rows.at[0:31], send_sem.at[6])
    left(ref_all.at[0 : zs - 1], send_sem.at[7])
    left(ids.at[1:4], send_sem.at[8])
    left(stat_quad, send_sem.at[9])
    left(stat_all.at[0 : zs - 1], send_sem.at[10])

    all_received(tot_all, 5)

    sums = functools.reduce(jnp.add, [tot_all[k] for k in range(32)])
    live_count, loss, kl, grads = [
        jnp.sum(jnp.where(lane == k, sums, 0.0), axis=1, keepdims=True) for k in range(4)
    ]
    sum_out[...] = jnp.where(
        lane == 0, loss / live_count, jnp.where(lane == 1, kl / live_count, jnp.sqrt(grads / live_count))
    )
    left(tot_all.at[0:31], send_sem.at[11])


def shards(hidden, norm_gain, head_weight, token_ids, lengths, old_logp, advantages, rollout_logp, rollout_row):
    tokens, features = hidden.shape
    rows_dev, cols = head_weight.shape
    zs = lax.axis_size("tensor")
    depth = features * zs
    vmem = pl.BlockSpec(memory_space=pltpu.VMEM)
    smem = pl.BlockSpec(memory_space=pltpu.SMEM)
    hbm = pl.BlockSpec(memory_space=pltpu.HBM)
    f32, bf16, i32 = jnp.float32, jnp.bfloat16, jnp.int32
    dma = pltpu.SemaphoreType.DMA
    new_logp, token_loss, summary = pl.pallas_call(
        kernel,
        out_shape=(
            jax.ShapeDtypeStruct((1, tokens), f32),
            jax.ShapeDtypeStruct((1, tokens), f32),
            jax.ShapeDtypeStruct((1, 128), f32),
        ),
        in_specs=[hbm, hbm, hbm, hbm, smem, hbm, hbm, hbm, smem],
        out_specs=(vmem, vmem, vmem),
        scratch_shapes=[
            pltpu.VMEM((CHUNKS, CHUNK, depth), bf16),
            pltpu.VMEM((2 * zs, tokens, features), bf16),
            pltpu.VMEM((4 * tokens, depth), bf16),
            pltpu.VMEM((4, 1, tokens), i32),
            pltpu.VMEM((1, 4 * tokens), i32),
            *[pltpu.VMEM((8, 4 * tokens), f32)] * 4,
            pltpu.VMEM((4, 16, 128), f32),
            pltpu.VMEM((3, 16, 128), f32),
            pltpu.VMEM((zs, 16, 128), f32),
            pltpu.VMEM((32, 1, 128), f32),
            pltpu.VMEM((zs, 1, 128), f32),
            pltpu.VMEM((zs, 1, features), f32),
            pltpu.VMEM((32, 1, 128), f32),
            pltpu.VMEM((features,), bf16),
            pltpu.VMEM((1, tokens), f32),
            pltpu.VMEM((1, tokens), f32),
            pltpu.VMEM((1, rollout_logp.shape[1]), f32),
            dma((6,)),
            dma((CHUNKS,)),
            dma((CHUNKS,)),
            dma((8, CHUNKS)),
            dma((2 * zs, SUBS)),
            dma((2, SUBS)),
            dma((zs,)),
            dma((6,)),
            dma((13,)),
        ],
        compiler_params=pltpu.CompilerParams(
            collective_id=0, has_side_effects=True, vmem_limit_bytes=64 * 1024 * 1024 - 256 * 1024
        ),
    )(
        hidden, norm_gain, head_weight.T, token_ids, lengths, old_logp, advantages, rollout_logp, rollout_row
    )
    return new_logp, token_loss, summary[0, :3]


def solution(mesh):
    in_specs = (
        P(("dp", "fsdp"), "tensor"),
        P("tensor"),
        P("fsdp", "tensor"),
        P(("dp", "fsdp"), None),
        P(("dp", "fsdp")),
        P(("dp", "fsdp"), None),
        P(("dp", "fsdp"), None),
        P(("dp", "fsdp"), "tensor"),
        P(("dp", "fsdp")),
    )
    out_specs = (P(("dp", "fsdp"), None), P(("dp", "fsdp"), None), P())
    return jax.shard_map(shards, mesh=mesh, in_specs=in_specs, out_specs=out_specs, check_vma=False)
```

```python
import collections
import functools
import heapq

import jax
import jax.numpy as jnp
from jax import lax
from jax.experimental import pallas as pl
from jax.experimental.pallas import tpu as pltpu
from jax.sharding import PartitionSpec as P

clip_eps = 0.2
kl_coef = 0.2
log_limit = 10.0
norm_eps = 1e-06

MESH = pl.DeviceIdType.MESH
LOW = -1e30
CHUNK = 256
SUB = 128
DEPTH = dict(z=2, l=2, y=2, h=2)
BATCH = 6
CHUNKS = 4
SUBS = 4
H_CUT, W_CUT = 1, 1
NEAR = (0, 2, 3, 5, 7)
TUNE = dict(y_far=-19.62, y_col=1.26, h_dy=(-3.37, -10.43, 17.88, -1.79), z_hop=1.73, z_sub=-12.0, z_late=31.14, l_hop=-29.7, l_sub=7.34, by_h=(3,))


def way_in(item):
    if item[0] == "w":
        _, col, dy, j = item
        if col == 0:
            if dy == 2:
                return "yp" if j < CHUNKS * W_CUT // 2 else "ym"
            return {0: None, 3: "yp", 1: "ym"}[dy]
        if dy in (0, 2) or j // W_CUT in TUNE["by_h"]:
            return "h"
        return "yp" if dy == 3 else "ym"
    _, who, dz, sub = item
    if who == 0 and dz == 0:
        return None
    if who == 1 and dz in NEAR:
        return "l"
    if dz == 4:
        return "zp" if sub < SUBS * H_CUT // 2 else "zm"
    return "zp" if dz > 4 else "zm"


def arrives_as(link, item):
    if item[0] == "w":
        _, col, dy, j = item
        if link == "h":
            return ("w", 1 - col, dy, j)
        return ("w", col, (dy + (3 if link == "yp" else 1)) % 4, j)
    _, who, dz, sub = item
    if link == "l":
        return ("h", 1 - who, dz, sub)
    return ("h", who, (dz + (7 if link == "zp" else 1)) % 8, sub)


def links_of(item):
    names = ("yp", "ym", "h") if item[0] == "w" else ("zp", "zm", "l")
    return [n for n in names if way_in(arrives_as(n, item)) == n]


def rank(link, item):
    t = TUNE
    if item[0] == "w":
        _, col, dy, j = item
        if link == "h":
            return (j / W_CUT + t["h_dy"][dy], dy)
        return (j / W_CUT + (t["y_far"] if dy else 0.0) + t["y_col"] * col, dy)
    _, who, dz, sub = item
    hops = min(dz, 8 - dz)
    if link == "l":
        return (hops * t["l_hop"] + sub / H_CUT * t["l_sub"], dz)
    return (hops * t["z_hop"] + sub / H_CUT * t["z_sub"] + who * t["z_late"], dz)


def plan():
    wire = {"w": 2.85 / W_CUT, "h": 1.43 / H_CUT}
    delay = 2.6
    norm_time, jobs_time, unit_time = 0.35, 0.15, 0.38
    names = ("zp", "zm", "l", "yp", "ym", "h")
    free = dict.fromkeys(names, 0.0)
    ends = {n: [] for n in names}
    ready = {n: [] for n in names}
    arrivals, ops = [], []
    for piece in range(SUBS * H_CUT):
        heapq.heappush(arrivals, (0.0, ("h", 0, 0, piece)))
    for piece in range(CHUNKS * W_CUT):
        heapq.heappush(arrivals, (1.0 + 0.2 * (piece // W_CUT), ("w", 0, 0, piece)))
    tokens = [(who, sub) for sub in range(SUBS) for who in (0, 1)]
    missing = {("c", j): 8 * W_CUT for j in range(CHUNKS)}
    missing.update({("n", *w): 8 * H_CUT for w in tokens})
    token_parts = {w: 2 for w in tokens}
    norms, units, chunks_here, tokens_here = [], [], [], []
    now = 0.0

    def top_up():
        for n in names:
            ends[n] = [e for e in ends[n] if e > now]
            while ready[n] and len(ends[n]) < DEPTH[n[0]]:
                _, item = heapq.heappop(ready[n])
                end = max(now, free[n]) + wire[item[0]]
                free[n] = end
                ends[n].append(end)
                ops.append(("send", n, item))
                heapq.heappush(arrivals, (end + delay, arrives_as(n, item)))

    def part_of(w):
        token_parts[w] -= 1
        if token_parts[w] == 0:
            tokens_here.append(w)
            units.extend((*w, j) for j in chunks_here)

    while arrivals or norms or units:
        if arrivals and arrivals[0][0] <= now:
            _, item = heapq.heappop(arrivals)
            ops.append(("wait", item))
            if item[0] == "p":
                part_of(item[1:])
                continue
            for n in links_of(item):
                heapq.heappush(ready[n], (rank(n, item), item))
            if not arrivals or arrivals[0][0] > now:
                top_up()
            key = ("c", item[3] // W_CUT) if item[0] == "w" else ("n", item[1], item[3] // H_CUT)
            missing[key] -= 1
            if missing[key] == 0:
                if key[0] == "c":
                    chunks_here.append(key[1])
                    units.extend((*w, key[1]) for w in tokens_here)
                else:
                    norms.append(key[1:])
        elif norms:
            who_sub = norms.pop(0)
            now += norm_time
            ops.append(("norm", who_sub))
            heapq.heappush(arrivals, (now + 1.8, ("p", *who_sub)))
            part_of(who_sub)
            top_up()
        elif units:
            units.sort(key=lambda unit: -unit[0])
            batch = [u for u in units if u[0] == units[0][0]][:BATCH]
            units = [u for u in units if u not in batch]
            batch.sort()
            now += jobs_time + unit_time * len(batch)
            ops.append(("jobs", tuple(batch)))
            top_up()
        else:
            now = arrivals[0][0]
            top_up()
    return ops


def kernel(
    hidden, gain_in, weight, ids_in, lens, old_in, adv_in, roll_in, row,
    out,
    w_all, hid, normed, ids, id_row, m_acc, s_acc, q_acc, p_acc,
    stat_rows, stat_quad, stat_all, ref_rows, ref_all, gains, tot_all, gain, old, adv, roll,
    local_sem, own_sem, wp_sem, w_sem, h_sem, n_sem, g_sem, all_sem, send_sem,
):
    lo, f, z = lax.axis_index("dp"), lax.axis_index("fsdp"), lax.axis_index("tensor")
    hi, y, c = f // 8, (f // 2) % 4, f % 2
    me = lo * 16 + f
    side = (lo + hi) % 2
    quarter = 2 * side + c
    cols, rows_dev = weight.shape
    zs, features = stat_all.shape[0], hid.shape[2]
    blocks = ids_in.shape[1] // 128
    last = cols - (4 * CHUNKS - 1) * CHUNK
    group = hi * 4 + y

    def at(hi_, lo_, y_, c_, z_):
        return {"dp": lo_, "fsdp": hi_ * 8 + y_ * 2 + c_, "tensor": z_}

    quad = [None, at(hi, lo, y, 1 - c, z), at(hi, 1 - lo, y, c, z), at(hi, 1 - lo, y, 1 - c, z)]
    partner = quad[1]
    target = {
        "yp": at(hi, lo, (y + 1) % 4, c, z),
        "ym": at(hi, lo, (y + 3) % 4, c, z),
        "h": at(1 - hi, 1 - lo, y, c, z),
        "l": quad[2],
        "zp": at(hi, lo, y, c, (z + 1) % zs),
        "zm": at(hi, lo, y, c, (z + zs - 1) % zs),
    }

    def plane_peer(k):
        other = (me + k) % 32
        return {"dp": other // 16, "fsdp": other % 16, "tensor": z}

    def line_peer(k):
        return {"dp": lo, "fsdp": f, "tensor": (z + k) % zs}

    def remote(src, dst, s, r, device):
        return pltpu.make_async_remote_copy(
            src_ref=src, dst_ref=dst, send_sem=s, recv_sem=r, device_id=device, device_id_type=MESH
        )

    def received(dst, r):
        remote(dst, dst, send_sem.at[0], r, partner).wait_recv()

    barrier = pltpu.get_barrier_semaphore()
    for device in (*quad[1:], *(target[n] for n in ("yp", "ym", "h", "zp", "zm"))):
        pl.semaphore_signal(barrier, inc=1, device_id=device, device_id_type=MESH)

    lane0 = pl.multiple_of(group * 256 + c * rows_dev, 128)

    def sized(j, owner, act):
        if j < CHUNKS - 1:
            act(CHUNK)
            return

        @pl.when(owner < 3)
        def _():
            act(CHUNK)

        @pl.when(owner == 3)
        def _():
            act(last)

    def own_weights(j, count):
        src = weight.at[pl.ds(pl.multiple_of((quarter * CHUNKS + j) * CHUNK, CHUNK), count), :]
        return pltpu.make_async_copy(src, w_all.at[j, pl.ds(0, count), pl.ds(lane0, 128)], own_sem.at[j])

    def pair_weights(j, count, owner):
        src = weight.at[pl.ds(pl.multiple_of((owner * CHUNKS + j) * CHUNK, CHUNK), count), :]
        dst = w_all.at[j, pl.ds(0, count), pl.ds(lane0, 128)]
        return remote(src, dst, send_sem.at[12 if j < CHUNKS - 1 else 0], wp_sem.at[j], partner)

    small = [
        pltpu.make_async_copy(src, dst, local_sem.at[k])
        for k, (src, dst) in enumerate(
            ((gain_in, gain), (roll_in, roll), (ids_in, ids.at[0]), (old_in, old), (adv_in, adv))
        )
    ]
    hid_in = pltpu.make_async_copy(hidden, hid.at[z], local_sem.at[7])
    hid_in.start()
    small[0].start()
    small[2].start()
    for j in range(CHUNKS):
        sized(j, quarter, lambda n, j=j: own_weights(j, n).start())
    for k in (1, 3, 4):
        small[k].start()

    @pl.when(quarter == 3)
    def _():
        pad = jnp.zeros((CHUNK - last, 256), jnp.bfloat16)
        w_all[CHUNKS - 1, last:CHUNK, pl.ds(pl.multiple_of(group * 256, 256), 256)] = pad

    lane = lax.broadcasted_iota(jnp.int32, (1, 128), 1)
    m_acc[...] = jnp.full(m_acc.shape, LOW, jnp.float32)
    s_acc[...] = jnp.zeros(s_acc.shape, jnp.float32)
    q_acc[...] = jnp.zeros(q_acc.shape, jnp.float32)
    p_acc[...] = jnp.zeros(p_acc.shape, jnp.float32)
    small[0].wait()
    gains[z] = gain[...].astype(jnp.float32).reshape(1, features)
    small[1].wait()
    ref_rows[0] = jnp.concatenate([roll[...], roll[...]], axis=1)
    small[2].wait()
    pl.semaphore_wait(barrier, 8)

    ops = plan()
    first_who, first_sub = next(op[1] for op in ops if op[0] == "norm")
    assert first_who == 0

    def w_piece(col, dy, j):
        g = (1 - hi if col else hi) * 4 + (y + dy) % 4
        return w_all.at[j, :, pl.ds(pl.multiple_of(g * 256, 256), 256)], w_sem.at[g, j]

    def h_piece(who, dz, sub):
        owner = who * zs + (z + dz) % zs
        return hid.at[owner, pl.ds(sub * SUB, SUB), :], h_sem.at[owner, sub]

    def with_gain(link, item):
        return link[0] == "z" and item[1] == 0 and item[3] == first_sub

    def send(link, item):
        if item[0] == "w":
            ref, sem = w_piece(*item[1:])
            remote(ref, ref, send_sem.at[1], sem, target[link]).start()
            return
        ref, sem = h_piece(*item[1:])
        other = h_piece(1 - item[1], *item[2:]) if link == "l" else (ref, sem)
        remote(ref, other[0], send_sem.at[2 if link == "l" else 3], other[1], target[link]).start()
        if with_gain(link, item):
            k = (z + item[2]) % zs
            remote(gains.at[k], gains.at[k], send_sem.at[4], g_sem.at[k], target[link]).start()

    def place(who, sub, core):
        return pl.multiple_of(((who * SUBS + sub) * 2 + core) * SUB, SUB)

    def wait(item):
        if item[0] == "p":
            received(normed.at[pl.ds(place(*item[1:], 1 - c), SUB), :], n_sem.at[item[1], item[2]])
        elif item[0] == "w" and item[1:3] == (0, 0):
            j = item[3]
            sized(j, quarter, lambda n: own_weights(j, n).wait())
            sized(j, quarter, lambda n: received(w_all.at[j, pl.ds(0, n), pl.ds(lane0, 128)], wp_sem.at[j]))
        elif item[0] == "w":
            received(*w_piece(*item[1:]))
        elif item[1:3] != (0, 0):
            received(*h_piece(*item[1:]))
            if item[1] == 0 and item[3] == first_sub:
                k = (z + item[2]) % zs
                received(gains.at[k], g_sem.at[k])

    def normalize(who, sub):
        gain_rows = [gains[k] for k in range(zs)]
        for t in range(0, SUB, 32):
            rows = slice(sub * SUB + t, sub * SUB + t + 32)
            squares = jnp.zeros((32, features), jnp.float32)
            for k in range(zs):
                part = hid[who * zs + k, rows, :].astype(jnp.float32)
                squares += part * part
            mean = jnp.sum(squares, axis=1, keepdims=True) * (1.0 / (zs * features))
            inv = lax.rsqrt(mean + norm_eps)
            out = pl.ds(pl.multiple_of(place(who, sub, c) + t, 32), 32)
            for k in range(zs):
                part = hid[who * zs + k, rows, :].astype(jnp.float32)
                normed[out, k * features : (k + 1) * features] = (part * inv * gain_rows[k]).astype(jnp.bfloat16)

        ref = normed.at[pl.ds(place(who, sub, c), SUB), :]
        remote(ref, ref, send_sem.at[5], n_sem.at[who, sub], partner).start()

    def job(who, sub, j):
        base = (quarter * CHUNKS + j) * CHUNK
        start = (who * SUBS + sub) * 2 * SUB
        tokens = slice(start, start + 2 * SUB)
        logits = lax.dot_general(
            w_all[j], normed[tokens, :], (((1,), (1,)), ((), ())), preferred_element_type=jnp.float32
        ).reshape(CHUNK // 8, 8, 2 * SUB)
        shape = (CHUNK // 8, 8, 1)
        column = lax.broadcasted_iota(jnp.int32, shape, 0) * 8 + lax.broadcasted_iota(jnp.int32, shape, 1)
        if j == CHUNKS - 1:
            logits = jnp.where(column < cols - base, logits, LOW)
        wanted = (id_row[:, tokens] - base)[None]
        p_acc[:, tokens] += jnp.sum(jnp.where(column == wanted, logits, 0.0), axis=0)
        old_max = m_acc[:, tokens]
        new_max = jnp.maximum(old_max, jnp.max(logits, axis=0))
        scale = jnp.exp(old_max - new_max)
        exps = jnp.exp(logits - new_max[None])
        s_acc[:, tokens] = s_acc[:, tokens] * scale + jnp.sum(exps, axis=0)
        q_acc[:, tokens] = q_acc[:, tokens] * (scale * scale) + jnp.sum(exps * exps, axis=0)
        m_acc[:, tokens] = new_max

    def ids_to_row():
        received(ids.at[1:4], all_sem.at[0])
        for s in range(4):
            for sub in range(SUBS):
                line = ids[s, :, sub * 128 : (sub + 1) * 128] - z * cols
                line = jnp.where((line >= 0) & (line < cols), line, -(1 << 20))
                id_row[:, pl.ds(place(s // 2, sub, (c + s) % 2), 128)] = line

    def share(who):
        tokens = slice(who * 2 * SUBS * SUB, (who + 1) * 2 * SUBS * SUB)
        top = jnp.max(m_acc[:, tokens], axis=0, keepdims=True)
        scale = jnp.exp(m_acc[:, tokens] - top)
        total = jnp.sum(s_acc[:, tokens] * scale, axis=0, keepdims=True)
        square = jnp.sum(q_acc[:, tokens] * (scale * scale), axis=0, keepdims=True)
        chosen = jnp.sum(p_acc[:, tokens], axis=0, keepdims=True)
        for core in (0, 1):
            starts = [(sub * 2 + core) * SUB for sub in range(SUBS)]
            stat_rows[who * 2 + (core + c) % 2] = jnp.concatenate(
                [value[:, i : i + SUB] for value in (top, total, square, chosen) for i in starts], axis=0
            )
        for s in (2, 3) if who else (1,):
            remote(stat_rows.at[s], stat_quad.at[s - 1], send_sem.at[9], all_sem.at[3], quad[s]).start()

    def to_plane(array, s, r):
        @pl.loop(0, 31)
        def _(i):
            k = (i + 15) % 31 + 1
            remote(array.at[0], array.at[k], send_sem.at[s], all_sem.at[r], plane_peer(k)).start()

    def to_line(array, s, r):
        for k in (4, 3, 5, 2, 6, 1, 7):
            remote(array.at[0], array.at[k], send_sem.at[s], all_sem.at[r], line_peer(k)).start()

    def all_received(array, r):
        received(array.at[1:], all_sem.at[r])

    def ref_start():
        to_plane(ref_rows, 6, 1)

    def ref_pick():
        all_received(ref_rows, 1)
        ref_all[0] = ref_rows[(me + 32 - row[0]) % 32]

    def ref_send():
        to_line(ref_all, 7, 2)

    def ref_wait():
        all_received(ref_all, 2)

    other = 2 * side + 1 - c
    for j in range(CHUNKS):
        sized(j, other, lambda n, j=j: pair_weights(j, n, other).start())
    for s in range(1, 4):
        remote(ids.at[0], ids.at[s], send_sem.at[8], all_sem.at[0], quad[s]).start()
    hid_in.wait()

    batches, neighbours_left = 0, SUBS * CHUNKS
    extra = {1: ref_start, 4: ref_pick, 5: ref_send, 8: ref_wait}
    for number, op in enumerate(ops):
        if op[0] == "send":
            send(op[1], op[2])
        elif op[0] == "wait":
            wait(op[1])
        elif op[0] == "norm":
            normalize(*op[1])
        else:
            for unit in op[1]:
                job(*unit)
                neighbours_left -= unit[0]
            if neighbours_left == 0:
                share(1)
                neighbours_left = -1
            batches += 1
            if batches in extra:
                extra[batches]()
        if number == 40:
            ids_to_row()

    share(0)
    received(stat_quad, all_sem.at[3])

    def merge(parts):
        top = functools.reduce(jnp.maximum, [p[0:4] for p in parts])
        total = square = chosen = 0.0
        for p in parts:
            scale = jnp.exp(p[0:4] - top)
            total += p[4:8] * scale
            square += p[8:12] * (scale * scale)
            chosen += p[12:16]
        return top, total, square, chosen

    stat_all[0] = jnp.concatenate(merge([stat_rows[0], *(stat_quad[s] for s in range(3))]), axis=0)

    to_line(stat_all, 10, 4)
    for k in (3, 4):
        small[k].wait()
    all_received(stat_all, 4)

    top, total, square, chosen = merge([stat_all[k] for k in range(zs)])
    new_logp = chosen - top - jnp.log(total)
    prob_square = square / (total * total)

    def lines(ref):
        return jnp.concatenate([ref[:, b * 128 : (b + 1) * 128] for b in range(blocks)], axis=0)

    old_logp, advantages = lines(old), lines(adv)
    ref_logp = jnp.concatenate(
        [jnp.where(lane < 64, ref_all[(z + zs - 2 * b) % zs], ref_all[(z + zs - 2 * b - 1) % zs]) for b in range(blocks)], axis=0
    )
    position = lax.broadcasted_iota(jnp.int32, (blocks, 128), 0) * 128 + lax.broadcasted_iota(
        jnp.int32, (blocks, 128), 1
    )
    live = jnp.where(position < lens[0], 1.0, 0.0)
    shift = new_logp - old_logp
    prob_ratio = jnp.exp(jnp.clip(shift, -log_limit, log_limit))
    clipped = jnp.clip(prob_ratio, 1.0 - clip_eps, 1.0 + clip_eps)
    plain_term = prob_ratio * advantages
    bounded_term = clipped * advantages
    surrogate = jnp.minimum(plain_term, bounded_term)
    ref_gap = ref_logp - new_logp
    gap_clip = jnp.clip(ref_gap, -log_limit, log_limit)
    gap_exp = jnp.exp(gap_clip)
    kl_term = gap_exp - gap_clip - 1.0
    token_loss = live * (kl_coef * kl_term - surrogate)
    inside_gap = jnp.where(jnp.abs(ref_gap) < log_limit, 1.0, 0.0)
    inside_ratio = jnp.where(jnp.abs(shift) < log_limit, 1.0, 0.0)
    active = jnp.where(plain_term <= bounded_term, 1.0, 0.0)
    grad = live * (kl_coef * (1.0 - gap_exp) * inside_gap - advantages * prob_ratio * active * inside_ratio)
    grad_square = grad * grad * (prob_square - 2.0 * jnp.exp(new_logp) + 1.0)

    def whole(array):
        return jnp.sum(jnp.sum(array, axis=0, keepdims=True), axis=1, keepdims=True)

    own_sums = jnp.zeros((1, 128), jnp.float32)
    for k, value in enumerate((live, token_loss, live * kl_term, grad_square)):
        own_sums = jnp.where(lane == k, whole(value), own_sums)
    tot_all[0] = own_sums

    to_plane(tot_all, 11, 5)

    for b in range(blocks):
        out[0:1, b * 128 : (b + 1) * 128] = new_logp[b : b + 1, :]
        out[1:2, b * 128 : (b + 1) * 128] = token_loss[b : b + 1, :]

    def left(src, sem):
        remote(src, src, sem, local_sem.at[0], partner).wait_send()

    left(weight.at[pl.ds(0, (CHUNKS - 1) * CHUNK), :], send_sem.at[12])
    sized(CHUNKS - 1, other, lambda n: left(weight.at[pl.ds(0, n), :], send_sem.at[0]))
    count = collections.Counter(
        op[1] if op[1] in ("l", "zp", "zm") else "w" for op in ops if op[0] == "send"
    )
    count["g"] = sum(op[0] == "send" and with_gain(op[1], op[2]) for op in ops)
    left(w_all.at[:, :, 0 : count["w"] // CHUNKS * 256], send_sem.at[1])
    left(hid.at[0 : count["l"] // SUBS], send_sem.at[2])
    left(hid.at[0 : (count["zp"] + count["zm"]) // SUBS], send_sem.at[3])
    left(gains.at[0 : count["g"]], send_sem.at[4])
    left(normed.at[0 : 2 * SUBS * SUB, :], send_sem.at[5])
    left(ref_rows.at[0:31], send_sem.at[6])
    left(ref_all.at[0 : zs - 1], send_sem.at[7])
    left(ids.at[1:4], send_sem.at[8])
    left(stat_quad, send_sem.at[9])
    left(stat_all.at[0 : zs - 1], send_sem.at[10])

    all_received(tot_all, 5)

    sums = functools.reduce(jnp.add, [tot_all[k] for k in range(32)])
    live_count, loss, kl, grads = [
        jnp.sum(jnp.where(lane == k, sums, 0.0), axis=1, keepdims=True) for k in range(4)
    ]
    out[2:3, 0:128] = jnp.where(
        lane == 0, loss / live_count, jnp.where(lane == 1, kl / live_count, jnp.sqrt(grads / live_count))
    )
    left(tot_all.at[0:31], send_sem.at[11])


def shards(hidden, norm_gain, head_weight, token_ids, lengths, old_logp, advantages, rollout_logp, rollout_row):
    tokens, features = hidden.shape
    rows_dev, cols = head_weight.shape
    zs = lax.axis_size("tensor")
    depth = features * zs
    hbm, smem = pl.BlockSpec(memory_space=pltpu.HBM), pl.BlockSpec(memory_space=pltpu.SMEM)
    f32, bf16, i32 = jnp.float32, jnp.bfloat16, jnp.int32
    dma = pltpu.SemaphoreType.DMA
    arrays = (hidden, norm_gain, head_weight.T, token_ids, lengths, old_logp, advantages, rollout_logp, rollout_row)
    packed = pl.pallas_call(
        kernel,
        out_shape=jax.ShapeDtypeStruct((8, tokens), f32),
        in_specs=[smem if a.size == 1 else hbm for a in arrays],
        out_specs=pl.BlockSpec(memory_space=pltpu.VMEM),
        scratch_shapes=[
            pltpu.VMEM((CHUNKS, CHUNK, depth), bf16),
            pltpu.VMEM((2 * zs, tokens, features), bf16),
            pltpu.VMEM((4 * tokens, depth), bf16),
            pltpu.VMEM((4, 1, tokens), i32),
            pltpu.VMEM((1, 4 * tokens), i32),
            *[pltpu.VMEM((8, 4 * tokens), f32)] * 4,
            pltpu.VMEM((4, 16, 128), f32),
            pltpu.VMEM((3, 16, 128), f32),
            pltpu.VMEM((zs, 16, 128), f32),
            pltpu.VMEM((32, 1, 128), f32),
            pltpu.VMEM((zs, 1, 128), f32),
            pltpu.VMEM((zs, 1, features), f32),
            pltpu.VMEM((32, 1, 128), f32),
            pltpu.VMEM((features,), bf16),
            pltpu.VMEM((1, tokens), f32),
            pltpu.VMEM((1, tokens), f32),
            pltpu.VMEM((1, rollout_logp.shape[1]), f32),
            dma((8,)),
            dma((CHUNKS,)),
            dma((CHUNKS,)),
            dma((8, CHUNKS)),
            dma((2 * zs, SUBS)),
            dma((2, SUBS)),
            dma((zs,)),
            dma((6,)),
            dma((13,)),
        ],
        compiler_params=pltpu.CompilerParams(
            collective_id=0, has_side_effects=True, vmem_limit_bytes=32 * 1024 * 1024
        ),
    )(
        *(a if a.size == 1 else pltpu.with_memory_space_constraint(a, pltpu.HBM) for a in arrays)
    )
    return packed[0:1], packed[1:2], packed[2, :3]


def solution(mesh):
    in_specs = (
        P(("dp", "fsdp"), "tensor"),
        P("tensor"),
        P("fsdp", "tensor"),
        P(("dp", "fsdp"), None),
        P(("dp", "fsdp")),
        P(("dp", "fsdp"), None),
        P(("dp", "fsdp"), None),
        P(("dp", "fsdp"), "tensor"),
        P(("dp", "fsdp")),
    )
    out_specs = (P(("dp", "fsdp"), None), P(("dp", "fsdp"), None), P())
    return jax.shard_map(shards, mesh=mesh, in_specs=in_specs, out_specs=out_specs, check_vma=False)
```

```python
import collections
import functools
import heapq

import jax
import jax.numpy as jnp
from jax import lax
from jax.experimental import pallas as pl
from jax.experimental.pallas import tpu as pltpu
from jax.sharding import PartitionSpec as P

clip_eps = 0.2
kl_coef = 0.2
log_limit = 10.0
norm_eps = 1e-06

MESH = pl.DeviceIdType.MESH
LOW = -1e30
CHUNK = 256
SUB = 128
DEPTH = dict(z=2, l=2, y=2, h=2)
BATCH = 6
CHUNKS = 4
SUBS = 4
H_CUT, W_CUT = 1, 1
NEAR = (0, 2, 3, 5, 7)
TUNE = dict(y_far=-19.62, y_col=1.26, h_dy=(-3.37, -10.43, 17.88, -1.79), z_hop=1.73, z_sub=-12.0, z_late=31.14, l_hop=-29.7, l_sub=7.34, by_h=(3,))


def way_in(item):
    if item[0] == "w":
        _, col, dy, j = item
        if col == 0:
            if dy == 2:
                return "yp" if j < CHUNKS * W_CUT // 2 else "ym"
            return {0: None, 3: "yp", 1: "ym"}[dy]
        if dy in (0, 2) or j // W_CUT in TUNE["by_h"]:
            return "h"
        return "yp" if dy == 3 else "ym"
    _, who, dz, sub = item
    if who == 0 and dz == 0:
        return None
    if who == 1 and dz in NEAR:
        return "l"
    if dz == 4:
        return "zp" if sub < SUBS * H_CUT // 2 else "zm"
    return "zp" if dz > 4 else "zm"


def arrives_as(link, item):
    if item[0] == "w":
        _, col, dy, j = item
        if link == "h":
            return ("w", 1 - col, dy, j)
        return ("w", col, (dy + (3 if link == "yp" else 1)) % 4, j)
    _, who, dz, sub = item
    if link == "l":
        return ("h", 1 - who, dz, sub)
    return ("h", who, (dz + (7 if link == "zp" else 1)) % 8, sub)


def links_of(item):
    names = ("yp", "ym", "h") if item[0] == "w" else ("zp", "zm", "l")
    return [n for n in names if way_in(arrives_as(n, item)) == n]


def rank(link, item):
    t = TUNE
    if item[0] == "w":
        _, col, dy, j = item
        if link == "h":
            return (j / W_CUT + t["h_dy"][dy], dy)
        return (j / W_CUT + (t["y_far"] if dy else 0.0) + t["y_col"] * col, dy)
    _, who, dz, sub = item
    hops = min(dz, 8 - dz)
    if link == "l":
        return (hops * t["l_hop"] + sub / H_CUT * t["l_sub"], dz)
    return (hops * t["z_hop"] + sub / H_CUT * t["z_sub"] + who * t["z_late"], dz)


def plan():
    wire = {"w": 2.85 / W_CUT, "h": 1.43 / H_CUT}
    delay = 2.3
    norm_time, jobs_time, unit_time = 0.35, 0.15, 0.38
    names = ("zp", "zm", "l", "yp", "ym", "h")
    free = dict.fromkeys(names, 0.0)
    ends = {n: [] for n in names}
    ready = {n: [] for n in names}
    arrivals, ops = [], []
    for piece in range(SUBS * H_CUT):
        heapq.heappush(arrivals, (0.0, ("h", 0, 0, piece)))
    for piece in range(CHUNKS * W_CUT):
        heapq.heappush(arrivals, (1.0 + 0.2 * (piece // W_CUT), ("w", 0, 0, piece)))
    tokens = [(who, sub) for sub in range(SUBS) for who in (0, 1)]
    missing = {("c", j): 8 * W_CUT for j in range(CHUNKS)}
    missing.update({("n", *w): 8 * H_CUT for w in tokens})
    token_parts = {w: 2 for w in tokens}
    norms, units, chunks_here, tokens_here = [], [], [], []
    now = 0.0

    def top_up():
        for n in names:
            ends[n] = [e for e in ends[n] if e > now]
            while ready[n] and len(ends[n]) < DEPTH[n[0]]:
                _, item = heapq.heappop(ready[n])
                end = max(now, free[n]) + wire[item[0]]
                free[n] = end
                ends[n].append(end)
                ops.append(("send", n, item))
                heapq.heappush(arrivals, (end + delay, arrives_as(n, item)))

    def part_of(w):
        token_parts[w] -= 1
        if token_parts[w] == 0:
            tokens_here.append(w)
            units.extend((*w, j) for j in chunks_here)

    while arrivals or norms or units:
        if arrivals and arrivals[0][0] <= now:
            _, item = heapq.heappop(arrivals)
            ops.append(("wait", item))
            if item[0] == "p":
                part_of(item[1:])
                continue
            for n in links_of(item):
                heapq.heappush(ready[n], (rank(n, item), item))
            if not arrivals or arrivals[0][0] > now:
                top_up()
            key = ("c", item[3] // W_CUT) if item[0] == "w" else ("n", item[1], item[3] // H_CUT)
            missing[key] -= 1
            if missing[key] == 0:
                if key[0] == "c":
                    chunks_here.append(key[1])
                    units.extend((*w, key[1]) for w in tokens_here)
                else:
                    norms.append(key[1:])
        elif norms:
            who_sub = norms.pop(0)
            now += norm_time
            ops.append(("norm", who_sub))
            heapq.heappush(arrivals, (now + 1.8, ("p", *who_sub)))
            part_of(who_sub)
            top_up()
        elif units:
            units.sort(key=lambda unit: -unit[0])
            batch = [u for u in units if u[0] == units[0][0]][:BATCH]
            units = [u for u in units if u not in batch]
            batch.sort()
            now += jobs_time + unit_time * len(batch)
            ops.append(("jobs", tuple(batch)))
            top_up()
        else:
            now = arrivals[0][0]
            top_up()
    return ops


def kernel(
    hidden, gain_in, weight, ids_in, lens, old_in, adv_in, roll_in, row,
    out,
    w_all, hid, normed, ids, id_row, m_acc, s_acc, q_acc, p_acc,
    stat_rows, stat_quad, stat_all, ref_rows, ref_all, gains, tot_all, gain, old, adv, roll,
    local_sem, own_sem, wp_sem, w_sem, h_sem, n_sem, g_sem, all_sem, send_sem, round_sem,
):
    lo, f, z = lax.axis_index("dp"), lax.axis_index("fsdp"), lax.axis_index("tensor")
    hi, y, c = f // 8, (f // 2) % 4, f % 2
    me = lo * 16 + f
    side = (lo + hi) % 2
    quarter = 2 * side + c
    cols, rows_dev = weight.shape
    zs, features = stat_all.shape[0], hid.shape[2]
    blocks = ids_in.shape[1] // 128
    last = cols - (4 * CHUNKS - 1) * CHUNK
    group = hi * 4 + y

    def at(hi_, lo_, y_, c_, z_):
        return {"dp": lo_, "fsdp": hi_ * 8 + y_ * 2 + c_, "tensor": z_}

    quad = [None, at(hi, lo, y, 1 - c, z), at(hi, 1 - lo, y, c, z), at(hi, 1 - lo, y, 1 - c, z)]
    partner = quad[1]
    target = {
        "yp": at(hi, lo, (y + 1) % 4, c, z),
        "ym": at(hi, lo, (y + 3) % 4, c, z),
        "h": at(1 - hi, 1 - lo, y, c, z),
        "l": quad[2],
        "zp": at(hi, lo, y, c, (z + 1) % zs),
        "zm": at(hi, lo, y, c, (z + zs - 1) % zs),
    }

    def plane_peer(k):
        other = lax.rem(me + k, 32)
        return {"dp": lax.div(other, 16), "fsdp": lax.rem(other, 16), "tensor": z}

    def line_peer(k):
        return {"dp": lo, "fsdp": f, "tensor": lax.rem(z + k, zs)}

    def remote(src, dst, s, r, device):
        return pltpu.make_async_remote_copy(
            src_ref=src, dst_ref=dst, send_sem=s, recv_sem=r, device_id=device, device_id_type=MESH
        )

    def received(dst, r):
        remote(dst, dst, send_sem.at[0], r, partner).wait_recv()

    barrier = pltpu.get_barrier_semaphore()
    for device in (*quad[1:], *(target[n] for n in ("yp", "ym", "h", "zp", "zm"))):
        pl.semaphore_signal(barrier, inc=1, device_id=device, device_id_type=MESH)

    lane0 = pl.multiple_of(group * 256 + c * rows_dev, 128)

    def sized(j, owner, act):
        if j < CHUNKS - 1:
            act(CHUNK)
            return

        @pl.when(owner < 3)
        def _():
            act(CHUNK)

        @pl.when(owner == 3)
        def _():
            act(last)

    def own_weights(j, count):
        src = weight.at[pl.ds(pl.multiple_of((quarter * CHUNKS + j) * CHUNK, CHUNK), count), :]
        return pltpu.make_async_copy(src, w_all.at[j, pl.ds(0, count), pl.ds(lane0, 128)], own_sem.at[j])

    def pair_weights(j, count, owner):
        src = weight.at[pl.ds(pl.multiple_of((owner * CHUNKS + j) * CHUNK, CHUNK), count), :]
        dst = w_all.at[j, pl.ds(0, count), pl.ds(lane0, 128)]
        return remote(src, dst, send_sem.at[12 if j < CHUNKS - 1 else 0], wp_sem.at[j], partner)

    small = [
        pltpu.make_async_copy(src, dst, local_sem.at[k])
        for k, (src, dst) in enumerate(
            ((gain_in, gain), (roll_in, roll), (ids_in, ids.at[0]), (old_in, old), (adv_in, adv))
        )
    ]
    hid_in = pltpu.make_async_copy(hidden, hid.at[z], local_sem.at[7])
    hid_in.start()
    small[0].start()
    small[2].start()
    for j in range(CHUNKS):
        sized(j, quarter, lambda n, j=j: own_weights(j, n).start())
    for k in (1, 3, 4):
        small[k].start()

    @pl.when(quarter == 3)
    def _():
        pad = jnp.zeros((CHUNK - last, 256), jnp.bfloat16)
        w_all[CHUNKS - 1, last:CHUNK, pl.ds(pl.multiple_of(group * 256, 256), 256)] = pad

    lane = lax.broadcasted_iota(jnp.int32, (1, 128), 1)
    m_acc[...] = jnp.full(m_acc.shape, LOW, jnp.float32)
    s_acc[...] = jnp.zeros(s_acc.shape, jnp.float32)
    q_acc[...] = jnp.zeros(q_acc.shape, jnp.float32)
    p_acc[...] = jnp.zeros(p_acc.shape, jnp.float32)
    small[0].wait()
    gains[z] = gain[...].astype(jnp.float32).reshape(1, features)
    small[1].wait()
    ref_rows[0] = jnp.concatenate([roll[...], roll[...]], axis=1)
    small[2].wait()
    pl.semaphore_wait(barrier, 8)

    ops = plan()
    first_who, first_sub = next(op[1] for op in ops if op[0] == "norm")
    assert first_who == 0

    def w_piece(col, dy, j):
        g = (1 - hi if col else hi) * 4 + (y + dy) % 4
        rows = CHUNK // W_CUT
        part = w_all.at[j // W_CUT, pl.ds(j % W_CUT * rows, rows), pl.ds(pl.multiple_of(g * 256, 256), 256)]
        return part, w_sem.at[g, j]

    def h_piece(who, dz, sub):
        owner = who * zs + (z + dz) % zs
        rows = SUB // H_CUT
        return hid.at[owner, pl.ds(sub * rows, rows), :], h_sem.at[owner, sub]

    def with_gain(link, item):
        return link[0] == "z" and item[1] == 0 and item[3] == first_sub * H_CUT

    def send(link, item):
        if item[0] == "w":
            ref, sem = w_piece(*item[1:])
            remote(ref, ref, send_sem.at[1], sem, target[link]).start()
            return
        ref, sem = h_piece(*item[1:])
        other = h_piece(1 - item[1], *item[2:]) if link == "l" else (ref, sem)
        remote(ref, other[0], send_sem.at[2 if link == "l" else 3], other[1], target[link]).start()
        if with_gain(link, item):
            k = (z + item[2]) % zs
            remote(gains.at[k], gains.at[k], send_sem.at[4], g_sem.at[k], target[link]).start()

    def place(who, sub, core):
        return pl.multiple_of(((who * SUBS + sub) * 2 + core) * SUB, SUB)

    def wait(item):
        if item[0] == "p":
            received(normed.at[pl.ds(place(*item[1:], 1 - c), SUB), :], n_sem.at[item[1], item[2]])
        elif item[0] == "w" and item[1:3] == (0, 0):
            if item[3] % W_CUT:
                return
            j = item[3] // W_CUT
            sized(j, quarter, lambda n: own_weights(j, n).wait())
            sized(j, quarter, lambda n: received(w_all.at[j, pl.ds(0, n), pl.ds(lane0, 128)], wp_sem.at[j]))
        elif item[0] == "w":
            received(*w_piece(*item[1:]))
        elif item[1:3] != (0, 0):
            received(*h_piece(*item[1:]))
            if item[1] == 0 and item[3] == first_sub * H_CUT:
                k = (z + item[2]) % zs
                received(gains.at[k], g_sem.at[k])

    def normalize(who, sub):
        gain_rows = [gains[k] for k in range(zs)]
        for t in range(0, SUB, 32):
            rows = slice(sub * SUB + t, sub * SUB + t + 32)
            squares = jnp.zeros((32, features), jnp.float32)
            for k in range(zs):
                part = hid[who * zs + k, rows, :].astype(jnp.float32)
                squares += part * part
            mean = jnp.sum(squares, axis=1, keepdims=True) * (1.0 / (zs * features))
            inv = lax.rsqrt(mean + norm_eps)
            out = pl.ds(pl.multiple_of(place(who, sub, c) + t, 32), 32)
            for k in range(zs):
                part = hid[who * zs + k, rows, :].astype(jnp.float32)
                normed[out, k * features : (k + 1) * features] = (part * inv * gain_rows[k]).astype(jnp.bfloat16)

        ref = normed.at[pl.ds(place(who, sub, c), SUB), :]
        remote(ref, ref, send_sem.at[5], n_sem.at[who, sub], partner).start()

    def job(who, sub, j, count):
        base = (quarter * CHUNKS + j) * CHUNK
        rows = count * CHUNK
        start = (who * SUBS + sub) * 2 * SUB
        tokens = slice(start, start + 2 * SUB)
        logits = lax.dot_general(
            w_all[j : j + count].reshape(rows, w_all.shape[2]),
            normed[tokens, :],
            (((1,), (1,)), ((), ())),
            preferred_element_type=jnp.float32,
        ).reshape(rows // 8, 8, 2 * SUB)
        shape = (rows // 8, 8, 1)
        column = lax.broadcasted_iota(jnp.int32, shape, 0) * 8 + lax.broadcasted_iota(jnp.int32, shape, 1)
        if j + count == CHUNKS:
            logits = jnp.where(column < cols - base, logits, LOW)
        wanted = (id_row[:, tokens] - base)[None]
        p_acc[:, tokens] += jnp.sum(jnp.where(column == wanted, logits, 0.0), axis=0)
        old_max = m_acc[:, tokens]
        new_max = jnp.maximum(old_max, jnp.max(logits, axis=0))
        scale = jnp.exp(old_max - new_max)
        exps = jnp.exp(logits - new_max[None])
        s_acc[:, tokens] = s_acc[:, tokens] * scale + jnp.sum(exps, axis=0)
        q_acc[:, tokens] = q_acc[:, tokens] * (scale * scale) + jnp.sum(exps * exps, axis=0)
        m_acc[:, tokens] = new_max

    def ids_to_row():
        received(ids.at[1:4], all_sem.at[0])
        for s in range(4):
            for sub in range(SUBS):
                line = ids[s, :, sub * 128 : (sub + 1) * 128] - z * cols
                line = jnp.where((line >= 0) & (line < cols), line, -(1 << 20))
                id_row[:, pl.ds(place(s // 2, sub, (c + s) % 2), 128)] = line

    def share(who):
        tokens = slice(who * 2 * SUBS * SUB, (who + 1) * 2 * SUBS * SUB)
        top = jnp.max(m_acc[:, tokens], axis=0, keepdims=True)
        scale = jnp.exp(m_acc[:, tokens] - top)
        total = jnp.sum(s_acc[:, tokens] * scale, axis=0, keepdims=True)
        square = jnp.sum(q_acc[:, tokens] * (scale * scale), axis=0, keepdims=True)
        chosen = jnp.sum(p_acc[:, tokens], axis=0, keepdims=True)
        for core in (0, 1):
            starts = [(sub * 2 + core) * SUB for sub in range(SUBS)]
            stat_rows[who * 2 + (core + c) % 2] = jnp.concatenate(
                [value[:, i : i + SUB] for value in (top, total, square, chosen) for i in starts], axis=0
            )
        for s in (2, 3) if who else (1,):
            remote(stat_rows.at[s], stat_quad.at[s - 1], send_sem.at[9], all_sem.at[3], quad[s]).start()

    def to_plane(array, s, r):
        @pl.loop(0, 31)
        def _(i):
            k = lax.rem(i + 15, 31) + 1
            remote(array.at[0], array.at[k], send_sem.at[s], all_sem.at[r], plane_peer(k)).start()

    def to_line(array, s, r):
        for k in (4, 3, 5, 2, 6, 1, 7):
            remote(array.at[0], array.at[k], send_sem.at[s], all_sem.at[r], line_peer(k)).start()

    def all_received(array, r):
        received(array.at[1:], all_sem.at[r])

    rounds = []

    def tell():
        rounds.append(len(rounds))
        for n in ("yp", "ym", "h"):
            pl.semaphore_signal(round_sem.at[rounds[-1]], inc=1, device_id=target[n], device_id_type=MESH)

    def hear():
        pl.semaphore_wait(round_sem.at[rounds[-1]], 3)

    def ref_start():
        to_plane(ref_rows, 6, 1)

    def ref_pick():
        all_received(ref_rows, 1)
        ref_all[0] = ref_rows[(me + 32 - row[0]) % 32]

    def ref_send():
        to_line(ref_all, 7, 2)

    def ref_wait():
        all_received(ref_all, 2)

    other = 2 * side + 1 - c
    for j in range(CHUNKS):
        sized(j, other, lambda n, j=j: pair_weights(j, n, other).start())
    for s in range(1, 4):
        remote(ids.at[0], ids.at[s], send_sem.at[8], all_sem.at[0], quad[s]).start()
    hid_in.wait()

    batches, neighbours_left = 0, SUBS * CHUNKS
    extra = {8: ref_wait}
    first_norm = next(number for number, op in enumerate(ops) if op[0] == "norm")
    early = {25: tell, 40: hear, 41: tell, 60: hear, 61: tell, 85: hear, 86: ref_start}
    early.update({first_norm - 1: ref_pick, first_norm: ref_send})
    for number, op in enumerate(ops):
        if op[0] == "send":
            send(op[1], op[2])
        elif op[0] == "wait":
            wait(op[1])
        elif op[0] == "norm":
            normalize(*op[1])
        else:
            for who, sub, j in op[1]:
                if (who, sub, j - 1) in op[1]:
                    continue
                count = 1
                while (who, sub, j + count) in op[1]:
                    count += 1
                job(who, sub, j, count)
            neighbours_left -= sum(unit[0] for unit in op[1])
            if neighbours_left == 0:
                share(1)
                neighbours_left = -1
            batches += 1
            if batches in extra:
                extra[batches]()
        if number == 40:
            ids_to_row()
        if number in early:
            early[number]()

    share(0)
    received(stat_quad, all_sem.at[3])

    def merge(parts):
        top = functools.reduce(jnp.maximum, [p[0:4] for p in parts])
        total = square = chosen = 0.0
        for p in parts:
            scale = jnp.exp(p[0:4] - top)
            total += p[4:8] * scale
            square += p[8:12] * (scale * scale)
            chosen += p[12:16]
        return top, total, square, chosen

    stat_all[0] = jnp.concatenate(merge([stat_rows[0], *(stat_quad[s] for s in range(3))]), axis=0)

    to_line(stat_all, 10, 4)
    for k in (3, 4):
        small[k].wait()
    all_received(stat_all, 4)

    top, total, square, chosen = merge([stat_all[k] for k in range(zs)])
    new_logp = chosen - top - jnp.log(total)
    prob_square = square / (total * total)

    def lines(ref):
        return jnp.concatenate([ref[:, b * 128 : (b + 1) * 128] for b in range(blocks)], axis=0)

    old_logp, advantages = lines(old), lines(adv)
    ref_logp = jnp.concatenate(
        [jnp.where(lane < 64, ref_all[(z + zs - 2 * b) % zs], ref_all[(z + zs - 2 * b - 1) % zs]) for b in range(blocks)], axis=0
    )
    position = lax.broadcasted_iota(jnp.int32, (blocks, 128), 0) * 128 + lax.broadcasted_iota(
        jnp.int32, (blocks, 128), 1
    )
    live = jnp.where(position < lens[0], 1.0, 0.0)
    shift = new_logp - old_logp
    prob_ratio = jnp.exp(jnp.clip(shift, -log_limit, log_limit))
    clipped = jnp.clip(prob_ratio, 1.0 - clip_eps, 1.0 + clip_eps)
    plain_term = prob_ratio * advantages
    bounded_term = clipped * advantages
    surrogate = jnp.minimum(plain_term, bounded_term)
    ref_gap = ref_logp - new_logp
    gap_clip = jnp.clip(ref_gap, -log_limit, log_limit)
    gap_exp = jnp.exp(gap_clip)
    kl_term = gap_exp - gap_clip - 1.0
    token_loss = live * (kl_coef * kl_term - surrogate)
    inside_gap = jnp.where(jnp.abs(ref_gap) < log_limit, 1.0, 0.0)
    inside_ratio = jnp.where(jnp.abs(shift) < log_limit, 1.0, 0.0)
    active = jnp.where(plain_term <= bounded_term, 1.0, 0.0)
    grad = live * (kl_coef * (1.0 - gap_exp) * inside_gap - advantages * prob_ratio * active * inside_ratio)
    grad_square = grad * grad * (prob_square - 2.0 * jnp.exp(new_logp) + 1.0)

    def whole(array):
        return jnp.sum(jnp.sum(array, axis=0, keepdims=True), axis=1, keepdims=True)

    own_sums = jnp.zeros((1, 128), jnp.float32)
    for k, value in enumerate((live, token_loss, live * kl_term, grad_square)):
        own_sums = jnp.where(lane == k, whole(value), own_sums)
    tot_all[0] = own_sums

    to_plane(tot_all, 11, 5)

    for b in range(blocks):
        out[0:1, b * 128 : (b + 1) * 128] = new_logp[b : b + 1, :]
        out[1:2, b * 128 : (b + 1) * 128] = token_loss[b : b + 1, :]

    def left(src, sem):
        remote(src, src, sem, local_sem.at[0], partner).wait_send()

    left(weight.at[pl.ds(0, (CHUNKS - 1) * CHUNK), :], send_sem.at[12])
    sized(CHUNKS - 1, other, lambda n: left(weight.at[pl.ds(0, n), :], send_sem.at[0]))
    count = collections.Counter(
        op[1] if op[1] in ("l", "zp", "zm") else "w" for op in ops if op[0] == "send"
    )
    count["g"] = sum(op[0] == "send" and with_gain(op[1], op[2]) for op in ops)
    left(w_all.at[:, :, 0 : count["w"] // (CHUNKS * W_CUT) * 256], send_sem.at[1])
    left(hid.at[0 : count["l"] // (SUBS * H_CUT)], send_sem.at[2])
    left(hid.at[0 : (count["zp"] + count["zm"]) // (SUBS * H_CUT)], send_sem.at[3])
    left(gains.at[0 : count["g"]], send_sem.at[4])
    left(normed.at[0 : 2 * SUBS * SUB, :], send_sem.at[5])
    left(ref_rows.at[0:31], send_sem.at[6])
    left(ref_all.at[0 : zs - 1], send_sem.at[7])
    left(ids.at[1:4], send_sem.at[8])
    left(stat_quad, send_sem.at[9])
    left(stat_all.at[0 : zs - 1], send_sem.at[10])

    all_received(tot_all, 5)

    sums = functools.reduce(jnp.add, [tot_all[k] for k in range(32)])
    live_count, loss, kl, grads = [
        jnp.sum(jnp.where(lane == k, sums, 0.0), axis=1, keepdims=True) for k in range(4)
    ]
    out[2:3, 0:128] = jnp.where(
        lane == 0, loss / live_count, jnp.where(lane == 1, kl / live_count, jnp.sqrt(grads / live_count))
    )
    left(tot_all.at[0:31], send_sem.at[11])


def shards(hidden, norm_gain, head_weight, token_ids, lengths, old_logp, advantages, rollout_logp, rollout_row):
    tokens, features = hidden.shape
    rows_dev, cols = head_weight.shape
    zs = lax.axis_size("tensor")
    depth = features * zs
    hbm, smem = pl.BlockSpec(memory_space=pltpu.HBM), pl.BlockSpec(memory_space=pltpu.SMEM)
    f32, bf16, i32 = jnp.float32, jnp.bfloat16, jnp.int32
    dma = pltpu.SemaphoreType.DMA
    arrays = (hidden, norm_gain, head_weight.T, token_ids, lengths, old_logp, advantages, rollout_logp, rollout_row)
    packed = pl.pallas_call(
        kernel,
        out_shape=jax.ShapeDtypeStruct((8, tokens), f32),
        in_specs=[smem if a.size == 1 else hbm for a in arrays],
        out_specs=pl.BlockSpec(memory_space=pltpu.VMEM),
        scratch_shapes=[
            pltpu.VMEM((CHUNKS, CHUNK, depth), bf16),
            pltpu.VMEM((2 * zs, tokens, features), bf16),
            pltpu.VMEM((4 * tokens, depth), bf16),
            pltpu.VMEM((4, 1, tokens), i32),
            pltpu.VMEM((1, 4 * tokens), i32),
            *[pltpu.VMEM((8, 4 * tokens), f32)] * 4,
            pltpu.VMEM((4, 16, 128), f32),
            pltpu.VMEM((3, 16, 128), f32),
            pltpu.VMEM((zs, 16, 128), f32),
            pltpu.VMEM((32, 1, 128), f32),
            pltpu.VMEM((zs, 1, 128), f32),
            pltpu.VMEM((zs, 1, features), f32),
            pltpu.VMEM((32, 1, 128), f32),
            pltpu.VMEM((features,), bf16),
            pltpu.VMEM((1, tokens), f32),
            pltpu.VMEM((1, tokens), f32),
            pltpu.VMEM((1, rollout_logp.shape[1]), f32),
            dma((8,)),
            dma((CHUNKS,)),
            dma((CHUNKS,)),
            dma((8, CHUNKS * W_CUT)),
            dma((2 * zs, SUBS * H_CUT)),
            dma((2, SUBS)),
            dma((zs,)),
            dma((6,)),
            dma((13,)),
            pltpu.SemaphoreType.REGULAR((3,)),
        ],
        compiler_params=pltpu.CompilerParams(
            collective_id=0, has_side_effects=True, vmem_limit_bytes=32 * 1024 * 1024
        ),
    )(
        *(a if a.size == 1 else pltpu.with_memory_space_constraint(a, pltpu.HBM) for a in arrays)
    )
    return packed[0:1], packed[1:2], packed[2, :3]


def solution(mesh):
    in_specs = (
        P(("dp", "fsdp"), "tensor"),
        P("tensor"),
        P("fsdp", "tensor"),
        P(("dp", "fsdp"), None),
        P(("dp", "fsdp")),
        P(("dp", "fsdp"), None),
        P(("dp", "fsdp"), None),
        P(("dp", "fsdp"), "tensor"),
        P(("dp", "fsdp")),
    )
    out_specs = (P(("dp", "fsdp"), None), P(("dp", "fsdp"), None), P())
    return jax.shard_map(shards, mesh=mesh, in_specs=in_specs, out_specs=out_specs, check_vma=False)
```

```python
import collections
import functools
import heapq

import jax
import jax.numpy as jnp
from jax import lax
from jax.experimental import pallas as pl
from jax.experimental.pallas import tpu as pltpu
from jax.sharding import PartitionSpec as P

clip_eps = 0.2
kl_coef = 0.2
log_limit = 10.0
norm_eps = 1e-06

MESH = pl.DeviceIdType.MESH
LOW = -1e30
CHUNK = 256
SUB = 128
DEPTH = dict(z=2, l=2, y=2, h=2)
BATCH = 6
CHUNKS = 4
SUBS = 4
H_CUT, W_CUT = 1, 1
NEAR = (0, 2, 3, 5, 7)
TUNE = dict(y_far=-19.62, y_col=1.26, h_dy=(-3.37, -10.43, 17.88, -1.79), z_hop=1.73, z_sub=-12.0, z_late=31.14, l_hop=-29.7, l_sub=7.34, by_h=(3,))


def way_in(item):
    if item[0] == "w":
        _, col, dy, j = item
        if col == 0:
            if dy == 2:
                return "yp" if j < CHUNKS * W_CUT // 2 else "ym"
            return {0: None, 3: "yp", 1: "ym"}[dy]
        if dy in (0, 2) or j // W_CUT in TUNE["by_h"]:
            return "h"
        return "yp" if dy == 3 else "ym"
    _, who, dz, sub = item
    if who == 0 and dz == 0:
        return None
    if who == 1 and dz in NEAR:
        return "l"
    if dz == 4:
        return "zp" if sub < SUBS * H_CUT // 2 else "zm"
    return "zp" if dz > 4 else "zm"


def arrives_as(link, item):
    if item[0] == "w":
        _, col, dy, j = item
        if link == "h":
            return ("w", 1 - col, dy, j)
        return ("w", col, (dy + (3 if link == "yp" else 1)) % 4, j)
    _, who, dz, sub = item
    if link == "l":
        return ("h", 1 - who, dz, sub)
    return ("h", who, (dz + (7 if link == "zp" else 1)) % 8, sub)


def links_of(item):
    names = ("yp", "ym", "h") if item[0] == "w" else ("zp", "zm", "l")
    return [n for n in names if way_in(arrives_as(n, item)) == n]


def rank(link, item):
    t = TUNE
    if item[0] == "w":
        _, col, dy, j = item
        if link == "h":
            return (j / W_CUT + t["h_dy"][dy], dy)
        return (j / W_CUT + (t["y_far"] if dy else 0.0) + t["y_col"] * col, dy)
    _, who, dz, sub = item
    hops = min(dz, 8 - dz)
    if link == "l":
        return (hops * t["l_hop"] + sub / H_CUT * t["l_sub"], dz)
    return (hops * t["z_hop"] + sub / H_CUT * t["z_sub"] + who * t["z_late"], dz)


def plan():
    wire = {"w": 2.85 / W_CUT, "h": 1.43 / H_CUT}
    delay = 2.3
    norm_time, jobs_time, unit_time = 0.35, 0.15, 0.38
    names = ("zp", "zm", "l", "yp", "ym", "h")
    free = dict.fromkeys(names, 0.0)
    ends = {n: [] for n in names}
    ready = {n: [] for n in names}
    arrivals, ops = [], []
    for piece in range(SUBS * H_CUT):
        heapq.heappush(arrivals, (0.0, ("h", 0, 0, piece)))
    for piece in range(CHUNKS * W_CUT):
        heapq.heappush(arrivals, (1.0 + 0.2 * (piece // W_CUT), ("w", 0, 0, piece)))
    tokens = [(who, sub) for sub in range(SUBS) for who in (0, 1)]
    missing = {("c", j): 8 * W_CUT for j in range(CHUNKS)}
    missing.update({("n", *w): 8 * H_CUT for w in tokens})
    token_parts = {w: 2 for w in tokens}
    norms, units, chunks_here, tokens_here = [], [], [], []
    now = 0.0

    def top_up():
        for n in names:
            ends[n] = [e for e in ends[n] if e > now]
            while ready[n] and len(ends[n]) < DEPTH[n[0]]:
                _, item = heapq.heappop(ready[n])
                end = max(now, free[n]) + wire[item[0]]
                free[n] = end
                ends[n].append(end)
                ops.append(("send", n, item))
                heapq.heappush(arrivals, (end + delay, arrives_as(n, item)))

    def part_of(w):
        token_parts[w] -= 1
        if token_parts[w] == 0:
            tokens_here.append(w)
            units.extend((*w, j) for j in chunks_here)

    while arrivals or norms or units:
        if arrivals and arrivals[0][0] <= now:
            _, item = heapq.heappop(arrivals)
            ops.append(("wait", item))
            if item[0] == "p":
                part_of(item[1:])
                continue
            for n in links_of(item):
                heapq.heappush(ready[n], (rank(n, item), item))
            if not arrivals or arrivals[0][0] > now:
                top_up()
            key = ("c", item[3] // W_CUT) if item[0] == "w" else ("n", item[1], item[3] // H_CUT)
            missing[key] -= 1
            if missing[key] == 0:
                if key[0] == "c":
                    chunks_here.append(key[1])
                    units.extend((*w, key[1]) for w in tokens_here)
                else:
                    norms.append(key[1:])
        elif norms:
            who_sub = norms.pop(0)
            now += norm_time
            ops.append(("norm", who_sub))
            heapq.heappush(arrivals, (now + 1.8, ("p", *who_sub)))
            part_of(who_sub)
            top_up()
        elif units:
            units.sort(key=lambda unit: -unit[0])
            batch = [u for u in units if u[0] == units[0][0]][:BATCH]
            units = [u for u in units if u not in batch]
            batch.sort()
            now += jobs_time + unit_time * len(batch)
            ops.append(("jobs", tuple(batch)))
            top_up()
        else:
            now = arrivals[0][0]
            top_up()
    return ops


def tidy(ops):
    out, held = [], ()
    for op in ops:
        if op[0] == "jobs":
            if len(op[1]) == 1 and out[-1][0] == "jobs":
                out[-1] = ("jobs", out[-1][1] + op[1])
                continue
            held += op[1]
            if len(held) == 1:
                continue
            op, held = ("jobs", held), ()
        out.append(op)
    return out + [("jobs", held)] * bool(held)


def kernel(
    hidden, gain_in, weight, ids_in, lens, old_in, adv_in, roll_in, row,
    out,
    w_all, hid, normed, ids, id_row, m_acc, s_acc, q_acc, p_acc,
    stat_rows, stat_quad, stat_all, ref_rows, ref_all, gains, tot_all, gain, old, adv, roll,
    local_sem, own_sem, wp_sem, w_sem, h_sem, n_sem, g_sem, all_sem, send_sem, round_sem,
):
    lo, f, z = lax.axis_index("dp"), lax.axis_index("fsdp"), lax.axis_index("tensor")
    hi, y, c = f // 8, (f // 2) % 4, f % 2
    me = lo * 16 + f
    side = (lo + hi) % 2
    quarter = 2 * side + c
    cols, rows_dev = weight.shape
    zs, features = stat_all.shape[0], hid.shape[2]
    blocks = ids_in.shape[1] // 128
    last = cols - (4 * CHUNKS - 1) * CHUNK
    group = hi * 4 + y

    def at(hi_, lo_, y_, c_, z_):
        return {"dp": lo_, "fsdp": hi_ * 8 + y_ * 2 + c_, "tensor": z_}

    quad = [None, at(hi, lo, y, 1 - c, z), at(hi, 1 - lo, y, c, z), at(hi, 1 - lo, y, 1 - c, z)]
    partner = quad[1]
    target = {
        "yp": at(hi, lo, (y + 1) % 4, c, z),
        "ym": at(hi, lo, (y + 3) % 4, c, z),
        "h": at(1 - hi, 1 - lo, y, c, z),
        "l": quad[2],
        "zp": at(hi, lo, y, c, (z + 1) % zs),
        "zm": at(hi, lo, y, c, (z + zs - 1) % zs),
    }

    def plane_peer(k):
        other = lax.rem(me + k, 32)
        return {"dp": lax.div(other, 16), "fsdp": lax.rem(other, 16), "tensor": z}

    def line_peer(k):
        return {"dp": lo, "fsdp": f, "tensor": lax.rem(z + k, zs)}

    def remote(src, dst, s, r, device):
        return pltpu.make_async_remote_copy(
            src_ref=src, dst_ref=dst, send_sem=s, recv_sem=r, device_id=device, device_id_type=MESH
        )

    def received(dst, r):
        remote(dst, dst, send_sem.at[0], r, partner).wait_recv()

    barrier = pltpu.get_barrier_semaphore()
    for device in (*quad[1:], *(target[n] for n in ("yp", "ym", "h", "zp", "zm"))):
        pl.semaphore_signal(barrier, inc=1, device_id=device, device_id_type=MESH)

    lane0 = pl.multiple_of(group * 256 + c * rows_dev, 128)

    def sized(j, owner, act):
        if j < CHUNKS - 1:
            act(CHUNK)
            return

        @pl.when(owner < 3)
        def _():
            act(CHUNK)

        @pl.when(owner == 3)
        def _():
            act(last)

    def own_weights(j, count):
        src = weight.at[pl.ds(pl.multiple_of((quarter * CHUNKS + j) * CHUNK, CHUNK), count), :]
        return pltpu.make_async_copy(src, w_all.at[j, pl.ds(0, count), pl.ds(lane0, 128)], own_sem.at[j])

    def pair_weights(j, count, owner):
        src = weight.at[pl.ds(pl.multiple_of((owner * CHUNKS + j) * CHUNK, CHUNK), count), :]
        dst = w_all.at[j, pl.ds(0, count), pl.ds(lane0, 128)]
        return remote(src, dst, send_sem.at[12 if j < CHUNKS - 1 else 0], wp_sem.at[j], partner)

    small = [
        pltpu.make_async_copy(src, dst, local_sem.at[k])
        for k, (src, dst) in enumerate(
            ((gain_in, gain), (roll_in, roll), (ids_in, ids.at[0]), (old_in, old), (adv_in, adv))
        )
    ]
    hid_in = pltpu.make_async_copy(hidden, hid.at[z], local_sem.at[7])
    hid_in.start()
    small[0].start()
    small[2].start()
    for j in range(CHUNKS):
        sized(j, quarter, lambda n, j=j: own_weights(j, n).start())
    for k in (1, 3, 4):
        small[k].start()

    @pl.when(quarter == 3)
    def _():
        pad = jnp.zeros((CHUNK - last, 256), jnp.bfloat16)
        w_all[CHUNKS - 1, last:CHUNK, pl.ds(pl.multiple_of(group * 256, 256), 256)] = pad

    lane = lax.broadcasted_iota(jnp.int32, (1, 128), 1)
    m_acc[...] = jnp.full(m_acc.shape, LOW, jnp.float32)
    s_acc[...] = jnp.zeros(s_acc.shape, jnp.float32)
    q_acc[...] = jnp.zeros(q_acc.shape, jnp.float32)
    p_acc[...] = jnp.zeros(p_acc.shape, jnp.float32)
    small[0].wait()
    gains[z] = gain[...].astype(jnp.float32).reshape(1, features)
    small[1].wait()
    ref_rows[0] = jnp.concatenate([roll[...], roll[...]], axis=1)
    small[2].wait()
    pl.semaphore_wait(barrier, 8)

    ops = tidy(plan())
    first_who, first_sub = next(op[1] for op in ops if op[0] == "norm")
    assert first_who == 0

    def w_piece(col, dy, j):
        g = (1 - hi if col else hi) * 4 + (y + dy) % 4
        rows = CHUNK // W_CUT
        part = w_all.at[j // W_CUT, pl.ds(j % W_CUT * rows, rows), pl.ds(pl.multiple_of(g * 256, 256), 256)]
        return part, w_sem.at[g, j]

    def h_piece(who, dz, sub):
        owner = who * zs + (z + dz) % zs
        rows = SUB // H_CUT
        return hid.at[owner, pl.ds(sub * rows, rows), :], h_sem.at[owner, sub]

    def with_gain(link, item):
        return link[0] == "z" and item[1] == 0 and item[3] == first_sub * H_CUT

    def send(link, item):
        if item[0] == "w":
            ref, sem = w_piece(*item[1:])
            remote(ref, ref, send_sem.at[1], sem, target[link]).start()
            return
        ref, sem = h_piece(*item[1:])
        other = h_piece(1 - item[1], *item[2:]) if link == "l" else (ref, sem)
        remote(ref, other[0], send_sem.at[2 if link == "l" else 3], other[1], target[link]).start()
        if with_gain(link, item):
            k = (z + item[2]) % zs
            remote(gains.at[k], gains.at[k], send_sem.at[4], g_sem.at[k], target[link]).start()

    def place(who, sub, core):
        return pl.multiple_of(((who * SUBS + sub) * 2 + core) * SUB, SUB)

    def wait(item):
        if item[0] == "p":
            received(normed.at[pl.ds(place(*item[1:], 1 - c), SUB), :], n_sem.at[item[1], item[2]])
        elif item[0] == "w" and item[1:3] == (0, 0):
            if item[3] % W_CUT:
                return
            j = item[3] // W_CUT
            sized(j, quarter, lambda n: own_weights(j, n).wait())
            sized(j, quarter, lambda n: received(w_all.at[j, pl.ds(0, n), pl.ds(lane0, 128)], wp_sem.at[j]))
        elif item[0] == "w":
            received(*w_piece(*item[1:]))
        elif item[1:3] != (0, 0):
            received(*h_piece(*item[1:]))
            if item[1] == 0 and item[3] == first_sub * H_CUT:
                k = (z + item[2]) % zs
                received(gains.at[k], g_sem.at[k])

    def normalize(who, sub):
        gain_rows = [gains[k] for k in range(zs)]
        for t in range(0, SUB, 32):
            rows = slice(sub * SUB + t, sub * SUB + t + 32)
            squares = jnp.zeros((32, features), jnp.float32)
            for k in range(zs):
                part = hid[who * zs + k, rows, :].astype(jnp.float32)
                squares += part * part
            mean = jnp.sum(squares, axis=1, keepdims=True) * (1.0 / (zs * features))
            inv = lax.rsqrt(mean + norm_eps)
            out = pl.ds(pl.multiple_of(place(who, sub, c) + t, 32), 32)
            for k in range(zs):
                part = hid[who * zs + k, rows, :].astype(jnp.float32)
                normed[out, k * features : (k + 1) * features] = (part * inv * gain_rows[k]).astype(jnp.bfloat16)

        ref = normed.at[pl.ds(place(who, sub, c), SUB), :]
        remote(ref, ref, send_sem.at[5], n_sem.at[who, sub], partner).start()

    def job(who, sub, j):
        base = (quarter * CHUNKS + j) * CHUNK
        start = (who * SUBS + sub) * 2 * SUB
        tokens = slice(start, start + 2 * SUB)
        logits = lax.dot_general(
            w_all[j], normed[tokens, :], (((1,), (1,)), ((), ())), preferred_element_type=jnp.float32
        ).reshape(CHUNK // 8, 8, 2 * SUB)
        shape = (CHUNK // 8, 8, 1)
        column = lax.broadcasted_iota(jnp.int32, shape, 0) * 8 + lax.broadcasted_iota(jnp.int32, shape, 1)
        if j == CHUNKS - 1:
            logits = jnp.where(column < cols - base, logits, LOW)
        wanted = (id_row[:, tokens] - base)[None]
        p_acc[:, tokens] += jnp.sum(jnp.where(column == wanted, logits, 0.0), axis=0)
        old_max = m_acc[:, tokens]
        new_max = jnp.maximum(old_max, jnp.max(logits, axis=0))
        scale = jnp.exp(old_max - new_max)
        exps = jnp.exp(logits - new_max[None])
        s_acc[:, tokens] = s_acc[:, tokens] * scale + jnp.sum(exps, axis=0)
        q_acc[:, tokens] = q_acc[:, tokens] * (scale * scale) + jnp.sum(exps * exps, axis=0)
        m_acc[:, tokens] = new_max

    def ids_to_row():
        received(ids.at[1:4], all_sem.at[0])
        for s in range(4):
            for sub in range(SUBS):
                line = ids[s, :, sub * 128 : (sub + 1) * 128] - z * cols
                line = jnp.where((line >= 0) & (line < cols), line, -(1 << 20))
                id_row[:, pl.ds(place(s // 2, sub, (c + s) % 2), 128)] = line

    def share(who):
        tokens = slice(who * 2 * SUBS * SUB, (who + 1) * 2 * SUBS * SUB)
        top = jnp.max(m_acc[:, tokens], axis=0, keepdims=True)
        scale = jnp.exp(m_acc[:, tokens] - top)
        total = jnp.sum(s_acc[:, tokens] * scale, axis=0, keepdims=True)
        square = jnp.sum(q_acc[:, tokens] * (scale * scale), axis=0, keepdims=True)
        chosen = jnp.sum(p_acc[:, tokens], axis=0, keepdims=True)
        for core in (0, 1):
            starts = [(sub * 2 + core) * SUB for sub in range(SUBS)]
            stat_rows[who * 2 + (core + c) % 2] = jnp.concatenate(
                [value[:, i : i + SUB] for value in (top, total, square, chosen) for i in starts], axis=0
            )
        for s in (2, 3) if who else (1,):
            remote(stat_rows.at[s], stat_quad.at[s - 1], send_sem.at[9], all_sem.at[3], quad[s]).start()

    def to_plane(array, s, r):
        @pl.loop(0, 31)
        def _(i):
            k = lax.rem(i + 15, 31) + 1
            remote(array.at[0], array.at[k], send_sem.at[s], all_sem.at[r], plane_peer(k)).start()

    def to_line(array, s, r):
        for k in (4, 3, 5, 2, 6, 1, 7):
            remote(array.at[0], array.at[k], send_sem.at[s], all_sem.at[r], line_peer(k)).start()

    def all_received(array, r):
        received(array.at[1:], all_sem.at[r])

    rounds = []

    def tell():
        rounds.append(len(rounds))
        for n in ("yp", "ym", "h"):
            pl.semaphore_signal(round_sem.at[rounds[-1]], inc=1, device_id=target[n], device_id_type=MESH)

    def hear():
        pl.semaphore_wait(round_sem.at[rounds[-1]], 3)

    def ref_start():
        to_plane(ref_rows, 6, 1)

    def ref_pick():
        all_received(ref_rows, 1)
        ref_all[0] = ref_rows[(me + 32 - row[0]) % 32]

    def ref_send():
        to_line(ref_all, 7, 2)

    def ref_wait():
        all_received(ref_all, 2)

    other = 2 * side + 1 - c
    for j in range(CHUNKS):
        sized(j, other, lambda n, j=j: pair_weights(j, n, other).start())
    for s in range(1, 4):
        remote(ids.at[0], ids.at[s], send_sem.at[8], all_sem.at[0], quad[s]).start()
    hid_in.wait()

    batches, neighbours_left = 0, SUBS * CHUNKS
    extra = {8: ref_wait}
    first_norm = next(number for number, op in enumerate(ops) if op[0] == "norm")
    early = {25: tell, 40: hear, 41: tell, 60: hear, 61: tell, 85: hear, 86: ref_start}
    early.update({first_norm - 1: ref_pick, first_norm: ref_send})
    for number, op in enumerate(ops):
        if op[0] == "send":
            send(op[1], op[2])
        elif op[0] == "wait":
            wait(op[1])
        elif op[0] == "norm":
            normalize(*op[1])
        else:
            for unit in op[1]:
                job(*unit)
            neighbours_left -= sum(unit[0] for unit in op[1])
            if neighbours_left == 0:
                share(1)
                neighbours_left = -1
            batches += 1
            if batches in extra:
                extra[batches]()
        if number == 40:
            ids_to_row()
        if number in early:
            early[number]()

    share(0)
    received(stat_quad, all_sem.at[3])

    def merge(parts):
        top = functools.reduce(jnp.maximum, [p[0:4] for p in parts])
        total = square = chosen = 0.0
        for p in parts:
            scale = jnp.exp(p[0:4] - top)
            total += p[4:8] * scale
            square += p[8:12] * (scale * scale)
            chosen += p[12:16]
        return top, total, square, chosen

    stat_all[0] = jnp.concatenate(merge([stat_rows[0], *(stat_quad[s] for s in range(3))]), axis=0)

    to_line(stat_all, 10, 4)
    for k in (3, 4):
        small[k].wait()
    all_received(stat_all, 4)

    top, total, square, chosen = merge([stat_all[k] for k in range(zs)])
    new_logp = chosen - top - jnp.log(total)
    prob_square = square / (total * total)

    def lines(ref):
        return jnp.concatenate([ref[:, b * 128 : (b + 1) * 128] for b in range(blocks)], axis=0)

    old_logp, advantages = lines(old), lines(adv)
    ref_logp = jnp.concatenate(
        [jnp.where(lane < 64, ref_all[(z + zs - 2 * b) % zs], ref_all[(z + zs - 2 * b - 1) % zs]) for b in range(blocks)], axis=0
    )
    position = lax.broadcasted_iota(jnp.int32, (blocks, 128), 0) * 128 + lax.broadcasted_iota(
        jnp.int32, (blocks, 128), 1
    )
    live = jnp.where(position < lens[0], 1.0, 0.0)
    shift = new_logp - old_logp
    prob_ratio = jnp.exp(jnp.clip(shift, -log_limit, log_limit))
    clipped = jnp.clip(prob_ratio, 1.0 - clip_eps, 1.0 + clip_eps)
    plain_term = prob_ratio * advantages
    bounded_term = clipped * advantages
    surrogate = jnp.minimum(plain_term, bounded_term)
    ref_gap = ref_logp - new_logp
    gap_clip = jnp.clip(ref_gap, -log_limit, log_limit)
    gap_exp = jnp.exp(gap_clip)
    kl_term = gap_exp - gap_clip - 1.0
    token_loss = live * (kl_coef * kl_term - surrogate)
    inside_gap = jnp.where(jnp.abs(ref_gap) < log_limit, 1.0, 0.0)
    inside_ratio = jnp.where(jnp.abs(shift) < log_limit, 1.0, 0.0)
    active = jnp.where(plain_term <= bounded_term, 1.0, 0.0)
    grad = live * (kl_coef * (1.0 - gap_exp) * inside_gap - advantages * prob_ratio * active * inside_ratio)
    grad_square = grad * grad * (prob_square - 2.0 * jnp.exp(new_logp) + 1.0)

    def whole(array):
        return jnp.sum(jnp.sum(array, axis=0, keepdims=True), axis=1, keepdims=True)

    own_sums = jnp.zeros((1, 128), jnp.float32)
    for k, value in enumerate((live, token_loss, live * kl_term, grad_square)):
        own_sums = jnp.where(lane == k, whole(value), own_sums)
    tot_all[0] = own_sums

    to_plane(tot_all, 11, 5)

    for b in range(blocks):
        out[0:1, b * 128 : (b + 1) * 128] = new_logp[b : b + 1, :]
        out[1:2, b * 128 : (b + 1) * 128] = token_loss[b : b + 1, :]

    def left(src, sem):
        remote(src, src, sem, local_sem.at[0], partner).wait_send()

    left(weight.at[pl.ds(0, (CHUNKS - 1) * CHUNK), :], send_sem.at[12])
    sized(CHUNKS - 1, other, lambda n: left(weight.at[pl.ds(0, n), :], send_sem.at[0]))
    count = collections.Counter(
        op[1] if op[1] in ("l", "zp", "zm") else "w" for op in ops if op[0] == "send"
    )
    count["g"] = sum(op[0] == "send" and with_gain(op[1], op[2]) for op in ops)
    left(w_all.at[:, :, 0 : count["w"] // (CHUNKS * W_CUT) * 256], send_sem.at[1])
    left(hid.at[0 : count["l"] // (SUBS * H_CUT)], send_sem.at[2])
    left(hid.at[0 : (count["zp"] + count["zm"]) // (SUBS * H_CUT)], send_sem.at[3])
    left(gains.at[0 : count["g"]], send_sem.at[4])
    left(normed.at[0 : 2 * SUBS * SUB, :], send_sem.at[5])
    left(ref_rows.at[0:31], send_sem.at[6])
    left(ref_all.at[0 : zs - 1], send_sem.at[7])
    left(ids.at[1:4], send_sem.at[8])
    left(stat_quad, send_sem.at[9])
    left(stat_all.at[0 : zs - 1], send_sem.at[10])

    all_received(tot_all, 5)

    sums = functools.reduce(jnp.add, [tot_all[k] for k in range(32)])
    live_count, loss, kl, grads = [
        jnp.sum(jnp.where(lane == k, sums, 0.0), axis=1, keepdims=True) for k in range(4)
    ]
    out[2:3, 0:128] = jnp.where(
        lane == 0, loss / live_count, jnp.where(lane == 1, kl / live_count, jnp.sqrt(grads / live_count))
    )
    left(tot_all.at[0:31], send_sem.at[11])


def shards(hidden, norm_gain, head_weight, token_ids, lengths, old_logp, advantages, rollout_logp, rollout_row):
    tokens, features = hidden.shape
    rows_dev, cols = head_weight.shape
    zs = lax.axis_size("tensor")
    depth = features * zs
    hbm, smem = pl.BlockSpec(memory_space=pltpu.HBM), pl.BlockSpec(memory_space=pltpu.SMEM)
    f32, bf16, i32 = jnp.float32, jnp.bfloat16, jnp.int32
    dma = pltpu.SemaphoreType.DMA
    arrays = (hidden, norm_gain, head_weight.T, token_ids, lengths, old_logp, advantages, rollout_logp, rollout_row)
    packed = pl.pallas_call(
        kernel,
        out_shape=jax.ShapeDtypeStruct((8, tokens), f32),
        in_specs=[smem if a.size == 1 else hbm for a in arrays],
        out_specs=pl.BlockSpec(memory_space=pltpu.VMEM),
        scratch_shapes=[
            pltpu.VMEM((CHUNKS, CHUNK, depth), bf16),
            pltpu.VMEM((2 * zs, tokens, features), bf16),
            pltpu.VMEM((4 * tokens, depth), bf16),
            pltpu.VMEM((4, 1, tokens), i32),
            pltpu.VMEM((1, 4 * tokens), i32),
            *[pltpu.VMEM((8, 4 * tokens), f32)] * 4,
            pltpu.VMEM((4, 16, 128), f32),
            pltpu.VMEM((3, 16, 128), f32),
            pltpu.VMEM((zs, 16, 128), f32),
            pltpu.VMEM((32, 1, 128), f32),
            pltpu.VMEM((zs, 1, 128), f32),
            pltpu.VMEM((zs, 1, features), f32),
            pltpu.VMEM((32, 1, 128), f32),
            pltpu.VMEM((features,), bf16),
            pltpu.VMEM((1, tokens), f32),
            pltpu.VMEM((1, tokens), f32),
            pltpu.VMEM((1, rollout_logp.shape[1]), f32),
            dma((8,)),
            dma((CHUNKS,)),
            dma((CHUNKS,)),
            dma((8, CHUNKS * W_CUT)),
            dma((2 * zs, SUBS * H_CUT)),
            dma((2, SUBS)),
            dma((zs,)),
            dma((6,)),
            dma((13,)),
            pltpu.SemaphoreType.REGULAR((3,)),
        ],
        compiler_params=pltpu.CompilerParams(
            collective_id=0, has_side_effects=True, vmem_limit_bytes=32 * 1024 * 1024
        ),
    )(
        *(a if a.size == 1 else pltpu.with_memory_space_constraint(a, pltpu.HBM) for a in arrays)
    )
    return packed[0:1], packed[1:2], packed[2, :3]


def solution(mesh):
    in_specs = (
        P(("dp", "fsdp"), "tensor"),
        P("tensor"),
        P("fsdp", "tensor"),
        P(("dp", "fsdp"), None),
        P(("dp", "fsdp")),
        P(("dp", "fsdp"), None),
        P(("dp", "fsdp"), None),
        P(("dp", "fsdp"), "tensor"),
        P(("dp", "fsdp")),
    )
    out_specs = (P(("dp", "fsdp"), None), P(("dp", "fsdp"), None), P())
    return jax.shard_map(shards, mesh=mesh, in_specs=in_specs, out_specs=out_specs, check_vma=False)
```

```python
import collections
import functools
import heapq

import jax
import jax.numpy as jnp
from jax import lax
from jax.experimental import pallas as pl
from jax.experimental.pallas import tpu as pltpu
from jax.sharding import PartitionSpec as P

clip_eps = 0.2
kl_coef = 0.2
log_limit = 10.0
norm_eps = 1e-06

MESH = pl.DeviceIdType.MESH
LOW = -1e30
CHUNK = 256
SUB = 128
DEPTH = dict(z=2, l=2, y=2, h=2)
BATCH = 6
CHUNKS = 4
SUBS = 4
H_CUT, W_CUT = 1, 1
NEAR = (0, 2, 3, 5, 7)
TUNE = dict(y_far=-19.62, y_col=1.26, h_dy=(-3.37, -10.43, 17.88, -1.79), z_hop=1.73, z_sub=-12.0, z_late=31.14, l_hop=-29.7, l_sub=7.34, by_h=(3,))


def way_in(item):
    if item[0] == "w":
        _, col, dy, j = item
        if col == 0:
            if dy == 2:
                return "yp" if j < CHUNKS * W_CUT // 2 else "ym"
            return {0: None, 3: "yp", 1: "ym"}[dy]
        if dy in (0, 2) or j // W_CUT in TUNE["by_h"]:
            return "h"
        return "yp" if dy == 3 else "ym"
    _, who, dz, sub = item
    if who == 0 and dz == 0:
        return None
    if who == 1 and dz in NEAR:
        return "l"
    if dz == 4:
        return "zp" if sub < SUBS * H_CUT // 2 else "zm"
    return "zp" if dz > 4 else "zm"


def arrives_as(link, item):
    if item[0] == "w":
        _, col, dy, j = item
        if link == "h":
            return ("w", 1 - col, dy, j)
        return ("w", col, (dy + (3 if link == "yp" else 1)) % 4, j)
    _, who, dz, sub = item
    if link == "l":
        return ("h", 1 - who, dz, sub)
    return ("h", who, (dz + (7 if link == "zp" else 1)) % 8, sub)


def links_of(item):
    names = ("yp", "ym", "h") if item[0] == "w" else ("zp", "zm", "l")
    return [n for n in names if way_in(arrives_as(n, item)) == n]


def rank(link, item):
    t = TUNE
    if item[0] == "w":
        _, col, dy, j = item
        if link == "h":
            return (j / W_CUT + t["h_dy"][dy], dy)
        return (j / W_CUT + (t["y_far"] if dy else 0.0) + t["y_col"] * col, dy)
    _, who, dz, sub = item
    hops = min(dz, 8 - dz)
    if link == "l":
        return (hops * t["l_hop"] + sub / H_CUT * t["l_sub"], dz)
    return (hops * t["z_hop"] + sub / H_CUT * t["z_sub"] + who * t["z_late"], dz)


def plan():
    wire = {"w": 2.85 / W_CUT, "h": 1.43 / H_CUT}
    delay = 2.3
    norm_time, jobs_time, unit_time = 0.35, 0.15, 0.38
    names = ("zp", "zm", "l", "yp", "ym", "h")
    free = dict.fromkeys(names, 0.0)
    ends = {n: [] for n in names}
    ready = {n: [] for n in names}
    arrivals, ops = [], []
    for piece in range(SUBS * H_CUT):
        heapq.heappush(arrivals, (0.0, ("h", 0, 0, piece)))
    for piece in range(CHUNKS * W_CUT):
        heapq.heappush(arrivals, (1.0 + 0.2 * (piece // W_CUT), ("w", 0, 0, piece)))
    tokens = [(who, sub) for sub in range(SUBS) for who in (0, 1)]
    missing = {("c", j): 8 * W_CUT for j in range(CHUNKS)}
    missing.update({("n", *w): 8 * H_CUT for w in tokens})
    token_parts = {w: 2 for w in tokens}
    norms, units, chunks_here, tokens_here = [], [], [], []
    now = 0.0

    def top_up():
        for n in names:
            ends[n] = [e for e in ends[n] if e > now]
            while ready[n] and len(ends[n]) < DEPTH[n[0]]:
                _, item = heapq.heappop(ready[n])
                end = max(now, free[n]) + wire[item[0]]
                free[n] = end
                ends[n].append(end)
                ops.append(("send", n, item))
                heapq.heappush(arrivals, (end + delay, arrives_as(n, item)))

    def part_of(w):
        token_parts[w] -= 1
        if token_parts[w] == 0:
            tokens_here.append(w)
            units.extend((*w, j) for j in chunks_here)

    while arrivals or norms or units:
        if arrivals and arrivals[0][0] <= now:
            _, item = heapq.heappop(arrivals)
            ops.append(("wait", item))
            if item[0] == "p":
                part_of(item[1:])
                continue
            for n in links_of(item):
                heapq.heappush(ready[n], (rank(n, item), item))
            if not arrivals or arrivals[0][0] > now:
                top_up()
            key = ("c", item[3] // W_CUT) if item[0] == "w" else ("n", item[1], item[3] // H_CUT)
            missing[key] -= 1
            if missing[key] == 0:
                if key[0] == "c":
                    chunks_here.append(key[1])
                    units.extend((*w, key[1]) for w in tokens_here)
                else:
                    norms.append(key[1:])
        elif norms:
            who_sub = norms.pop(0)
            now += norm_time
            ops.append(("norm", who_sub))
            heapq.heappush(arrivals, (now + 1.8, ("p", *who_sub)))
            part_of(who_sub)
            top_up()
        elif units:
            units.sort(key=lambda unit: -unit[0])
            batch = [u for u in units if u[0] == units[0][0]][:BATCH]
            units = [u for u in units if u not in batch]
            batch.sort()
            now += jobs_time + unit_time * len(batch)
            ops.append(("jobs", tuple(batch)))
            top_up()
        else:
            now = arrivals[0][0]
            top_up()
    return ops


def late_waits(ops):
    out, pending = [], collections.defaultdict(list)
    for op in ops:
        needs = []
        if op[0] == "wait":
            item = op[1]
            if item[0] == "p" or not links_of(item):
                key = ("w", item[3]) if item[0] == "w" else (item[0], item[1], item[-1])
                pending[key].append(op)
                continue
        elif op[0] == "norm":
            needs = [("h", *op[1])]
        elif op[0] == "jobs":
            needs = [key for unit in op[1] for key in (("p", *unit[:2]), ("w", unit[2]))]
        for key in needs:
            out.extend(pending.pop(key, ()))
        out.append(op)
    assert not any(pending.values())
    return out


def kernel(
    hidden, gain_in, weight, ids_in, lens, old_in, adv_in, roll_in, row,
    out,
    w_all, hid, normed, ids, id_row, m_acc, s_acc, q_acc, p_acc,
    stat_rows, stat_quad, stat_all, ref_rows, ref_all, gains, tot_all, gain, old, adv, roll,
    local_sem, own_sem, wp_sem, w_sem, h_sem, n_sem, g_sem, all_sem, send_sem, round_sem,
):
    lo, f, z = lax.axis_index("dp"), lax.axis_index("fsdp"), lax.axis_index("tensor")
    hi, y, c = f // 8, (f // 2) % 4, f % 2
    me = lo * 16 + f
    side = (lo + hi) % 2
    quarter = 2 * side + c
    cols, rows_dev = weight.shape
    zs, features = stat_all.shape[0], hid.shape[2]
    blocks = ids_in.shape[1] // 128
    last = cols - (4 * CHUNKS - 1) * CHUNK
    group = hi * 4 + y

    def at(hi_, lo_, y_, c_, z_):
        return {"dp": lo_, "fsdp": hi_ * 8 + y_ * 2 + c_, "tensor": z_}

    quad = [None, at(hi, lo, y, 1 - c, z), at(hi, 1 - lo, y, c, z), at(hi, 1 - lo, y, 1 - c, z)]
    partner = quad[1]
    target = {
        "yp": at(hi, lo, (y + 1) % 4, c, z),
        "ym": at(hi, lo, (y + 3) % 4, c, z),
        "h": at(1 - hi, 1 - lo, y, c, z),
        "l": quad[2],
        "zp": at(hi, lo, y, c, (z + 1) % zs),
        "zm": at(hi, lo, y, c, (z + zs - 1) % zs),
    }

    def plane_peer(k):
        other = lax.rem(me + k, 32)
        return {"dp": lax.div(other, 16), "fsdp": lax.rem(other, 16), "tensor": z}

    def line_peer(k):
        return {"dp": lo, "fsdp": f, "tensor": lax.rem(z + k, zs)}

    def remote(src, dst, s, r, device):
        return pltpu.make_async_remote_copy(
            src_ref=src, dst_ref=dst, send_sem=s, recv_sem=r, device_id=device, device_id_type=MESH
        )

    def received(dst, r):
        remote(dst, dst, send_sem.at[0], r, partner).wait_recv()

    barrier = pltpu.get_barrier_semaphore()
    for device in (*quad[1:], *(target[n] for n in ("yp", "ym", "h", "zp", "zm"))):
        pl.semaphore_signal(barrier, inc=1, device_id=device, device_id_type=MESH)

    lane0 = pl.multiple_of(group * 256 + c * rows_dev, 128)

    def sized(j, owner, act):
        if j < CHUNKS - 1:
            act(CHUNK)
            return

        @pl.when(owner < 3)
        def _():
            act(CHUNK)

        @pl.when(owner == 3)
        def _():
            act(last)

    def own_weights(j, count):
        src = weight.at[pl.ds(pl.multiple_of((quarter * CHUNKS + j) * CHUNK, CHUNK), count), :]
        return pltpu.make_async_copy(src, w_all.at[j, pl.ds(0, count), pl.ds(lane0, 128)], own_sem.at[j])

    def pair_weights(j, count, owner):
        src = weight.at[pl.ds(pl.multiple_of((owner * CHUNKS + j) * CHUNK, CHUNK), count), :]
        dst = w_all.at[j, pl.ds(0, count), pl.ds(lane0, 128)]
        return remote(src, dst, send_sem.at[12 if j < CHUNKS - 1 else 0], wp_sem.at[j], partner)

    small = [
        pltpu.make_async_copy(src, dst, local_sem.at[k])
        for k, (src, dst) in enumerate(
            ((gain_in, gain), (roll_in, roll), (ids_in, ids.at[0]), (old_in, old), (adv_in, adv))
        )
    ]
    hid_in = pltpu.make_async_copy(hidden, hid.at[z], local_sem.at[7])
    hid_in.start()
    small[0].start()
    small[2].start()
    for j in range(CHUNKS):
        sized(j, quarter, lambda n, j=j: own_weights(j, n).start())
    for k in (1, 3, 4):
        small[k].start()

    @pl.when(quarter == 3)
    def _():
        pad = jnp.zeros((CHUNK - last, 256), jnp.bfloat16)
        w_all[CHUNKS - 1, last:CHUNK, pl.ds(pl.multiple_of(group * 256, 256), 256)] = pad

    lane = lax.broadcasted_iota(jnp.int32, (1, 128), 1)
    m_acc[...] = jnp.full(m_acc.shape, LOW, jnp.float32)
    s_acc[...] = jnp.zeros(s_acc.shape, jnp.float32)
    q_acc[...] = jnp.zeros(q_acc.shape, jnp.float32)
    p_acc[...] = jnp.zeros(p_acc.shape, jnp.float32)
    small[0].wait()
    gains[z] = gain[...].astype(jnp.float32).reshape(1, features)
    small[1].wait()
    ref_rows[0] = jnp.concatenate([roll[...], roll[...]], axis=1)
    small[2].wait()
    pl.semaphore_wait(barrier, 8)

    ops = late_waits(plan())
    first_who, first_sub = next(op[1] for op in ops if op[0] == "norm")
    assert first_who == 0

    def w_piece(col, dy, j):
        g = (1 - hi if col else hi) * 4 + (y + dy) % 4
        rows = CHUNK // W_CUT
        part = w_all.at[j // W_CUT, pl.ds(j % W_CUT * rows, rows), pl.ds(pl.multiple_of(g * 256, 256), 256)]
        return part, w_sem.at[g, j]

    def h_piece(who, dz, sub):
        owner = who * zs + (z + dz) % zs
        rows = SUB // H_CUT
        return hid.at[owner, pl.ds(sub * rows, rows), :], h_sem.at[owner, sub]

    def with_gain(link, item):
        return link[0] == "z" and item[1] == 0 and item[3] == first_sub * H_CUT

    def send(link, item):
        if item[0] == "w":
            ref, sem = w_piece(*item[1:])
            remote(ref, ref, send_sem.at[1], sem, target[link]).start()
            return
        ref, sem = h_piece(*item[1:])
        other = h_piece(1 - item[1], *item[2:]) if link == "l" else (ref, sem)
        remote(ref, other[0], send_sem.at[2 if link == "l" else 3], other[1], target[link]).start()
        if with_gain(link, item):
            k = (z + item[2]) % zs
            remote(gains.at[k], gains.at[k], send_sem.at[4], g_sem.at[k], target[link]).start()

    def place(who, sub, core):
        return pl.multiple_of(((who * SUBS + sub) * 2 + core) * SUB, SUB)

    def wait(item):
        if item[0] == "p":
            received(normed.at[pl.ds(place(*item[1:], 1 - c), SUB), :], n_sem.at[item[1], item[2]])
        elif item[0] == "w" and item[1:3] == (0, 0):
            if item[3] % W_CUT:
                return
            j = item[3] // W_CUT
            sized(j, quarter, lambda n: own_weights(j, n).wait())
            sized(j, quarter, lambda n: received(w_all.at[j, pl.ds(0, n), pl.ds(lane0, 128)], wp_sem.at[j]))
        elif item[0] == "w":
            received(*w_piece(*item[1:]))
        elif item[1:3] != (0, 0):
            received(*h_piece(*item[1:]))
            if item[1] == 0 and item[3] == first_sub * H_CUT:
                k = (z + item[2]) % zs
                received(gains.at[k], g_sem.at[k])

    def normalize(who, sub):
        gain_rows = [gains[k] for k in range(zs)]
        for t in range(0, SUB, 32):
            rows = slice(sub * SUB + t, sub * SUB + t + 32)
            squares = jnp.zeros((32, features), jnp.float32)
            for k in range(zs):
                part = hid[who * zs + k, rows, :].astype(jnp.float32)
                squares += part * part
            mean = jnp.sum(squares, axis=1, keepdims=True) * (1.0 / (zs * features))
            inv = lax.rsqrt(mean + norm_eps)
            out = pl.ds(pl.multiple_of(place(who, sub, c) + t, 32), 32)
            for k in range(zs):
                part = hid[who * zs + k, rows, :].astype(jnp.float32)
                normed[out, k * features : (k + 1) * features] = (part * inv * gain_rows[k]).astype(jnp.bfloat16)

        ref = normed.at[pl.ds(place(who, sub, c), SUB), :]
        remote(ref, ref, send_sem.at[5], n_sem.at[who, sub], partner).start()

    def job(who, sub, j):
        base = (quarter * CHUNKS + j) * CHUNK
        start = (who * SUBS + sub) * 2 * SUB
        tokens = slice(start, start + 2 * SUB)
        logits = lax.dot_general(
            w_all[j], normed[tokens, :], (((1,), (1,)), ((), ())), preferred_element_type=jnp.float32
        ).reshape(CHUNK // 8, 8, 2 * SUB)
        shape = (CHUNK // 8, 8, 1)
        column = lax.broadcasted_iota(jnp.int32, shape, 0) * 8 + lax.broadcasted_iota(jnp.int32, shape, 1)
        if j == CHUNKS - 1:
            logits = jnp.where(column < cols - base, logits, LOW)
        wanted = (id_row[:, tokens] - base)[None]
        p_acc[:, tokens] += jnp.sum(jnp.where(column == wanted, logits, 0.0), axis=0)
        old_max = m_acc[:, tokens]
        new_max = jnp.maximum(old_max, jnp.max(logits, axis=0))
        scale = jnp.exp(old_max - new_max)
        exps = jnp.exp(logits - new_max[None])
        s_acc[:, tokens] = s_acc[:, tokens] * scale + jnp.sum(exps, axis=0)
        q_acc[:, tokens] = q_acc[:, tokens] * (scale * scale) + jnp.sum(exps * exps, axis=0)
        m_acc[:, tokens] = new_max

    def ids_to_row():
        received(ids.at[1:4], all_sem.at[0])
        for s in range(4):
            for sub in range(SUBS):
                line = ids[s, :, sub * 128 : (sub + 1) * 128] - z * cols
                line = jnp.where((line >= 0) & (line < cols), line, -(1 << 20))
                id_row[:, pl.ds(place(s // 2, sub, (c + s) % 2), 128)] = line

    def share(who):
        tokens = slice(who * 2 * SUBS * SUB, (who + 1) * 2 * SUBS * SUB)
        top = jnp.max(m_acc[:, tokens], axis=0, keepdims=True)
        scale = jnp.exp(m_acc[:, tokens] - top)
        total = jnp.sum(s_acc[:, tokens] * scale, axis=0, keepdims=True)
        square = jnp.sum(q_acc[:, tokens] * (scale * scale), axis=0, keepdims=True)
        chosen = jnp.sum(p_acc[:, tokens], axis=0, keepdims=True)
        for core in (0, 1):
            starts = [(sub * 2 + core) * SUB for sub in range(SUBS)]
            stat_rows[who * 2 + (core + c) % 2] = jnp.concatenate(
                [value[:, i : i + SUB] for value in (top, total, square, chosen) for i in starts], axis=0
            )
        for s in (2, 3) if who else (1,):
            remote(stat_rows.at[s], stat_quad.at[s - 1], send_sem.at[9], all_sem.at[3], quad[s]).start()

    def to_plane(array, s, r):
        @pl.loop(0, 31)
        def _(i):
            k = lax.rem(i + 15, 31) + 1
            remote(array.at[0], array.at[k], send_sem.at[s], all_sem.at[r], plane_peer(k)).start()

    def to_line(array, s, r):
        for k in (4, 3, 5, 2, 6, 1, 7):
            remote(array.at[0], array.at[k], send_sem.at[s], all_sem.at[r], line_peer(k)).start()

    def all_received(array, r):
        received(array.at[1:], all_sem.at[r])

    rounds = []

    def tell():
        rounds.append(len(rounds))
        for n in ("yp", "ym", "h"):
            pl.semaphore_signal(round_sem.at[rounds[-1]], inc=1, device_id=target[n], device_id_type=MESH)

    def hear():
        pl.semaphore_wait(round_sem.at[rounds[-1]], 3)

    def ref_start():
        to_plane(ref_rows, 6, 1)

    def ref_pick():
        all_received(ref_rows, 1)
        ref_all[0] = ref_rows[(me + 32 - row[0]) % 32]

    def ref_send():
        to_line(ref_all, 7, 2)

    def ref_wait():
        all_received(ref_all, 2)

    other = 2 * side + 1 - c
    for j in range(CHUNKS):
        sized(j, other, lambda n, j=j: pair_weights(j, n, other).start())
    for s in range(1, 4):
        remote(ids.at[0], ids.at[s], send_sem.at[8], all_sem.at[0], quad[s]).start()
    hid_in.wait()

    batches, neighbours_left = 0, SUBS * CHUNKS
    extra = {8: ref_wait}
    first_norm = next(number for number, op in enumerate(ops) if op[0] == "norm")
    early = {25: tell, 40: hear, 41: tell, 60: hear, 61: tell, 85: hear, 86: ref_start}
    early.update({first_norm - 1: ref_pick, first_norm: ref_send})
    for number, op in enumerate(ops):
        if op[0] == "send":
            send(op[1], op[2])
        elif op[0] == "wait":
            wait(op[1])
        elif op[0] == "norm":
            normalize(*op[1])
        else:
            for unit in op[1]:
                job(*unit)
            neighbours_left -= sum(unit[0] for unit in op[1])
            if neighbours_left == 0:
                share(1)
                neighbours_left = -1
            batches += 1
            if batches in extra:
                extra[batches]()
        if number == 40:
            ids_to_row()
        if number in early:
            early[number]()

    share(0)
    received(stat_quad, all_sem.at[3])

    def merge(parts):
        top = functools.reduce(jnp.maximum, [p[0:4] for p in parts])
        total = square = chosen = 0.0
        for p in parts:
            scale = jnp.exp(p[0:4] - top)
            total += p[4:8] * scale
            square += p[8:12] * (scale * scale)
            chosen += p[12:16]
        return top, total, square, chosen

    stat_all[0] = jnp.concatenate(merge([stat_rows[0], *(stat_quad[s] for s in range(3))]), axis=0)

    to_line(stat_all, 10, 4)
    for k in (3, 4):
        small[k].wait()
    all_received(stat_all, 4)

    top, total, square, chosen = merge([stat_all[k] for k in range(zs)])
    new_logp = chosen - top - jnp.log(total)
    prob_square = square / (total * total)

    def lines(ref):
        return jnp.concatenate([ref[:, b * 128 : (b + 1) * 128] for b in range(blocks)], axis=0)

    old_logp, advantages = lines(old), lines(adv)
    ref_logp = jnp.concatenate(
        [jnp.where(lane < 64, ref_all[(z + zs - 2 * b) % zs], ref_all[(z + zs - 2 * b - 1) % zs]) for b in range(blocks)], axis=0
    )
    position = lax.broadcasted_iota(jnp.int32, (blocks, 128), 0) * 128 + lax.broadcasted_iota(
        jnp.int32, (blocks, 128), 1
    )
    live = jnp.where(position < lens[0], 1.0, 0.0)
    shift = new_logp - old_logp
    prob_ratio = jnp.exp(jnp.clip(shift, -log_limit, log_limit))
    clipped = jnp.clip(prob_ratio, 1.0 - clip_eps, 1.0 + clip_eps)
    plain_term = prob_ratio * advantages
    bounded_term = clipped * advantages
    surrogate = jnp.minimum(plain_term, bounded_term)
    ref_gap = ref_logp - new_logp
    gap_clip = jnp.clip(ref_gap, -log_limit, log_limit)
    gap_exp = jnp.exp(gap_clip)
    kl_term = gap_exp - gap_clip - 1.0
    token_loss = live * (kl_coef * kl_term - surrogate)
    inside_gap = jnp.where(jnp.abs(ref_gap) < log_limit, 1.0, 0.0)
    inside_ratio = jnp.where(jnp.abs(shift) < log_limit, 1.0, 0.0)
    active = jnp.where(plain_term <= bounded_term, 1.0, 0.0)
    grad = live * (kl_coef * (1.0 - gap_exp) * inside_gap - advantages * prob_ratio * active * inside_ratio)
    grad_square = grad * grad * (prob_square - 2.0 * jnp.exp(new_logp) + 1.0)

    def whole(array):
        return jnp.sum(jnp.sum(array, axis=0, keepdims=True), axis=1, keepdims=True)

    own_sums = jnp.zeros((1, 128), jnp.float32)
    for k, value in enumerate((live, token_loss, live * kl_term, grad_square)):
        own_sums = jnp.where(lane == k, whole(value), own_sums)
    tot_all[0] = own_sums

    to_plane(tot_all, 11, 5)

    for b in range(blocks):
        out[0:1, b * 128 : (b + 1) * 128] = new_logp[b : b + 1, :]
        out[1:2, b * 128 : (b + 1) * 128] = token_loss[b : b + 1, :]

    def left(src, sem):
        remote(src, src, sem, local_sem.at[0], partner).wait_send()

    left(weight.at[pl.ds(0, (CHUNKS - 1) * CHUNK), :], send_sem.at[12])
    sized(CHUNKS - 1, other, lambda n: left(weight.at[pl.ds(0, n), :], send_sem.at[0]))
    count = collections.Counter(
        op[1] if op[1] in ("l", "zp", "zm") else "w" for op in ops if op[0] == "send"
    )
    count["g"] = sum(op[0] == "send" and with_gain(op[1], op[2]) for op in ops)
    left(w_all.at[:, :, 0 : count["w"] // (CHUNKS * W_CUT) * 256], send_sem.at[1])
    left(hid.at[0 : count["l"] // (SUBS * H_CUT)], send_sem.at[2])
    left(hid.at[0 : (count["zp"] + count["zm"]) // (SUBS * H_CUT)], send_sem.at[3])
    left(gains.at[0 : count["g"]], send_sem.at[4])
    left(normed.at[0 : 2 * SUBS * SUB, :], send_sem.at[5])
    left(ref_rows.at[0:31], send_sem.at[6])
    left(ref_all.at[0 : zs - 1], send_sem.at[7])
    left(ids.at[1:4], send_sem.at[8])
    left(stat_quad, send_sem.at[9])
    left(stat_all.at[0 : zs - 1], send_sem.at[10])

    all_received(tot_all, 5)

    sums = functools.reduce(jnp.add, [tot_all[k] for k in range(32)])
    live_count, loss, kl, grads = [
        jnp.sum(jnp.where(lane == k, sums, 0.0), axis=1, keepdims=True) for k in range(4)
    ]
    out[2:3, 0:128] = jnp.where(
        lane == 0, loss / live_count, jnp.where(lane == 1, kl / live_count, jnp.sqrt(grads / live_count))
    )
    left(tot_all.at[0:31], send_sem.at[11])


def shards(hidden, norm_gain, head_weight, token_ids, lengths, old_logp, advantages, rollout_logp, rollout_row):
    tokens, features = hidden.shape
    rows_dev, cols = head_weight.shape
    zs = lax.axis_size("tensor")
    depth = features * zs
    hbm, smem = pl.BlockSpec(memory_space=pltpu.HBM), pl.BlockSpec(memory_space=pltpu.SMEM)
    f32, bf16, i32 = jnp.float32, jnp.bfloat16, jnp.int32
    dma = pltpu.SemaphoreType.DMA
    arrays = (hidden, norm_gain, head_weight.T, token_ids, lengths, old_logp, advantages, rollout_logp, rollout_row)
    packed = pl.pallas_call(
        kernel,
        out_shape=jax.ShapeDtypeStruct((8, tokens), f32),
        in_specs=[smem if a.size == 1 else hbm for a in arrays],
        out_specs=pl.BlockSpec(memory_space=pltpu.VMEM),
        scratch_shapes=[
            pltpu.VMEM((CHUNKS, CHUNK, depth), bf16),
            pltpu.VMEM((2 * zs, tokens, features), bf16),
            pltpu.VMEM((4 * tokens, depth), bf16),
            pltpu.VMEM((4, 1, tokens), i32),
            pltpu.VMEM((1, 4 * tokens), i32),
            *[pltpu.VMEM((8, 4 * tokens), f32)] * 4,
            pltpu.VMEM((4, 16, 128), f32),
            pltpu.VMEM((3, 16, 128), f32),
            pltpu.VMEM((zs, 16, 128), f32),
            pltpu.VMEM((32, 1, 128), f32),
            pltpu.VMEM((zs, 1, 128), f32),
            pltpu.VMEM((zs, 1, features), f32),
            pltpu.VMEM((32, 1, 128), f32),
            pltpu.VMEM((features,), bf16),
            pltpu.VMEM((1, tokens), f32),
            pltpu.VMEM((1, tokens), f32),
            pltpu.VMEM((1, rollout_logp.shape[1]), f32),
            dma((8,)),
            dma((CHUNKS,)),
            dma((CHUNKS,)),
            dma((8, CHUNKS * W_CUT)),
            dma((2 * zs, SUBS * H_CUT)),
            dma((2, SUBS)),
            dma((zs,)),
            dma((6,)),
            dma((13,)),
            pltpu.SemaphoreType.REGULAR((3,)),
        ],
        compiler_params=pltpu.CompilerParams(
            collective_id=0, has_side_effects=True, vmem_limit_bytes=32 * 1024 * 1024
        ),
    )(
        *(a if a.size == 1 else pltpu.with_memory_space_constraint(a, pltpu.HBM) for a in arrays)
    )
    return packed[0:1], packed[1:2], packed[2, :3]


def solution(mesh):
    in_specs = (
        P(("dp", "fsdp"), "tensor"),
        P("tensor"),
        P("fsdp", "tensor"),
        P(("dp", "fsdp"), None),
        P(("dp", "fsdp")),
        P(("dp", "fsdp"), None),
        P(("dp", "fsdp"), None),
        P(("dp", "fsdp"), "tensor"),
        P(("dp", "fsdp")),
    )
    out_specs = (P(("dp", "fsdp"), None), P(("dp", "fsdp"), None), P())
    return jax.shard_map(shards, mesh=mesh, in_specs=in_specs, out_specs=out_specs, check_vma=False)
```
